32 devices in a mesh: dp: 4 (over z), expert: 2 (over x), tensor: 4 (over y, core).
Axes of the slice: x: 2, y: 2, z: 4, core: 2. Of those that a mesh axis runs over, the one named last changes fastest.
Arguments:
- tokens: bfloat16 [256, 4096], P(('dp', 'expert', 'tensor')), may hold values from -6 to 6
- out_grad: bfloat16 [256, 4096], P(('dp', 'expert', 'tensor')), may hold values from -4 to 4
- route_probs: float32 [256, 2], P(('dp', 'expert')), may hold values from 0.2 to 1
- expert_ids: int32 [256, 2], P(('dp', 'expert')), may hold values from 0 to 7, as said below
- slot_index: int32 [256, 2], P(('dp', 'expert')), may hold values from 0 to 10, as said below
- w_gate: bfloat16 [8, 4096, 7168], P('expert', 'dp', 'tensor'), may hold values from -0.09375 to 0.09375
- w_up: bfloat16 [8, 4096, 7168], P('expert', 'dp', 'tensor'), may hold values from -0.09375 to 0.09375
- w_down: bfloat16 [8, 7168, 4096], P('expert', 'tensor', 'dp'), may hold values from -0.0625 to 0.0625
Outputs:
- token_grad: bfloat16 [256, 4096], P(('dp', 'expert', 'tensor'))
- grad_gate: bfloat16 [8, 4096, 7168], P('expert', 'dp', 'tensor')
- grad_up: bfloat16 [8, 4096, 7168], P('expert', 'dp', 'tensor')
- grad_down: bfloat16 [8, 7168, 4096], P('expert', 'tensor', 'dp')
The draws below stay inside these ranges and needn't reach their ends.
Inputs may be any that keep to these rules, and one draw needn't show every extreme that they name: `expert_ids`: the 2 entries of a token are different experts. slot_index[t, k] counts the earlier routes to expert_ids[t, k] within the token's routing block of 32 rows, in order of tokens and then of routes; the value 10 marks a route past the capacity, which is dropped (a count of 10 or more is given as 10). In every draw some expert is filled to 10 slots in every block.
All inputs are finite; a program needn't handle non-finite values.
Results may differ from the reference program's by a relative error of at most 0.011.
Values may be sent and summed in bfloat16 or wider, within the bound.
A program may use at most 192 MiB of HBM per device.

```python
import jax
import jax.numpy as jnp
from jax import lax

D = 4096
EXPERTS = 8
TOP = 2
FF = 7168
GROUP = 32
CAP = 10
TOKENS = 256


def route_draw(key):
    blocks = TOKENS // GROUP
    base = jax.random.fold_in(key, 7)
    hot_key, pick_key, first_key, second_key = jax.random.split(base, 4)
    hot_expert = jax.random.randint(hot_key, (), 0, EXPERTS)
    pick = jax.random.randint(pick_key, (blocks, GROUP), 0, 2)
    first_any = jax.random.randint(first_key, (blocks, GROUP), 0, EXPERTS)
    first = jnp.where(pick == 1, hot_expert, first_any)
    second = (first + 1 + jax.random.randint(second_key, (blocks, GROUP), 0, EXPERTS - 1)) % EXPERTS
    chosen = jnp.stack([first, second], -1).astype(jnp.int32)
    flat_ids = chosen.reshape(blocks, GROUP * TOP)
    onehot = (flat_ids[:, :, None] == jnp.arange(EXPERTS, dtype=jnp.int32)[None, None, :]).astype(jnp.int32)
    earlier = jnp.cumsum(onehot, axis=1) - onehot
    position = jnp.sum(earlier * onehot, axis=-1)
    position = jnp.minimum(position, CAP).astype(jnp.int32)
    return (chosen.reshape(TOKENS, TOP), position.reshape(TOKENS, TOP))


def draw_expert_ids(key, part):
    return route_draw(key)[0]


def draw_slot_index(key, part):
    return route_draw(key)[1]


def level_of(rng, shape, cuts, low, largest):
    def one(axis_at, blocks):
        steps = jax.random.uniform(jax.random.fold_in(jax.random.fold_in(rng, 6), axis_at), (blocks,), jnp.float32, low / len(cuts), largest / len(cuts))
        return jnp.repeat(jnp.exp(steps), shape[axis_at] // blocks).reshape((-1,) + (1,) * (len(shape) - axis_at - 1))

    gain = one(*cuts[0])
    for cut in cuts[1:]:
        gain = gain * one(*cut)
    return gain


def scatter_about(own_key, extent, spread, most, cuts=(), kind=jnp.bfloat16):
    values = jax.random.normal(own_key, extent, jnp.float32) * spread
    if len(cuts) > 0:
        values = level_of(own_key, extent, cuts, -0.22, 0.18) * values
    return jnp.clip(values, min=-most, max=most).astype(kind)


def setup_inputs(seed: int = 0) -> dict:
    key_of = jax.random.split(jax.random.key(seed), 9)
    return {
        "tokens": scatter_about(key_of[0], (TOKENS, D), 1.0, 6.0, ((0, 32),)),
        "out_grad": scatter_about(key_of[1], (TOKENS, D), 0.5, 4.0, ((0, 32),)),
        "route_probs": jnp.clip(0.2 + 0.8 * jax.random.uniform(key_of[2], (TOKENS, TOP), jnp.float32) ** level_of(key_of[2], (TOKENS, TOP), ((0, 8),), -0.2, 0.2), 0.2, 1.0),
        "expert_ids": draw_expert_ids(jax.random.fold_in(key_of[8], 71), 0),
        "slot_index": draw_slot_index(jax.random.fold_in(key_of[8], 71), 0),
        "w_gate": scatter_about(key_of[5], (EXPERTS, D, FF), D ** -0.5, 0.09375, ((0, 2), (1, 4), (2, 4))),
        "w_up": scatter_about(key_of[6], (EXPERTS, D, FF), D ** -0.5, 0.09375, ((0, 2), (1, 4), (2, 4))),
        "w_down": scatter_about(key_of[7], (EXPERTS, FF, D), FF ** -0.5, 0.0625, ((0, 2), (1, 4), (2, 4))),
    }


def route_tables(expert_ids, slot_index, capacity):
    target = slot_index * EXPERTS + expert_ids
    target = jnp.where(slot_index < capacity, target, -1).astype(jnp.int32)
    places = jnp.arange(capacity * EXPERTS, dtype=jnp.int32)
    return [(places[:, None] == target[None, :, k]).astype(jnp.bfloat16) for k in range(TOP)]


def swiglu_back(pre_gate, pre_up, grad_hidden):
    sigmoid_gate = jax.nn.sigmoid(pre_gate)
    silu_gate = pre_gate * sigmoid_gate
    hidden = (silu_gate * pre_up).astype(jnp.bfloat16)
    up_delta = (grad_hidden * silu_gate).astype(jnp.bfloat16)
    gate_delta = (grad_hidden * pre_up * sigmoid_gate * (1.0 + pre_gate * (1.0 - sigmoid_gate))).astype(jnp.bfloat16)
    return hidden, gate_delta, up_delta


def reference(tokens, out_grad, route_probs, expert_ids, slot_index, w_gate, w_up, w_down):
    blocks = TOKENS // GROUP
    capacity = CAP

    def dispatch(inputs):
        block_x, block_dy, block_probs, block_ids, block_slots = inputs
        tables = route_tables(block_ids, block_slots, capacity)
        table_sum = tables[0] + tables[1]
        x_buf = jnp.dot(table_sum, block_x, preferred_element_type=jnp.float32).astype(jnp.bfloat16)
        grad_buf = jnp.zeros((capacity * EXPERTS, D), jnp.float32)
        for k in range(TOP):
            scaled = (block_probs[:, k:k + 1] * block_dy.astype(jnp.float32)).astype(jnp.bfloat16)
            grad_buf = grad_buf + jnp.dot(tables[k], scaled, preferred_element_type=jnp.float32)
        grad_buf = grad_buf.astype(jnp.bfloat16)
        return (x_buf.reshape(capacity, EXPERTS, D), grad_buf.reshape(capacity, EXPERTS, D),
                table_sum.astype(jnp.float32))

    x_bufs, grad_bufs, table_all = lax.map(dispatch, (
        tokens.reshape(blocks, GROUP, D), out_grad.reshape(blocks, GROUP, D),
        route_probs.reshape(blocks, GROUP, TOP), expert_ids.reshape(blocks, GROUP, TOP),
        slot_index.reshape(blocks, GROUP, TOP)))
    expert_x = jnp.moveaxis(x_bufs, 2, 0).reshape(EXPERTS, blocks * capacity, D)
    expert_g = jnp.moveaxis(grad_bufs, 2, 0).reshape(EXPERTS, blocks * capacity, D)

    def expert_back(inputs):
        rows_x, rows_g, gate_w, up_w, down_w = inputs
        pre_gate = jnp.dot(rows_x, gate_w, preferred_element_type=jnp.float32)
        pre_up = jnp.dot(rows_x, up_w, preferred_element_type=jnp.float32)
        grad_hidden = jnp.dot(rows_g, down_w.T, preferred_element_type=jnp.float32)
        hidden, gate_delta, up_delta = swiglu_back(pre_gate, pre_up, grad_hidden)
        g_down = jnp.dot(hidden.T, rows_g, preferred_element_type=jnp.float32).astype(jnp.bfloat16)
        g_gate = jnp.dot(rows_x.T, gate_delta, preferred_element_type=jnp.float32).astype(jnp.bfloat16)
        g_up = jnp.dot(rows_x.T, up_delta, preferred_element_type=jnp.float32).astype(jnp.bfloat16)
        row_grad = jnp.dot(gate_delta, gate_w.T, preferred_element_type=jnp.float32)
        row_grad = row_grad + jnp.dot(up_delta, up_w.T, preferred_element_type=jnp.float32)
        return g_gate, g_up, g_down, row_grad

    grad_gate, grad_up, grad_down, row_grad = lax.map(expert_back, (expert_x, expert_g, w_gate, w_up, w_down))
    row_grad = row_grad.reshape(EXPERTS, blocks, capacity, D)
    row_grad = jnp.transpose(row_grad, (1, 2, 0, 3)).reshape(blocks, capacity * EXPERTS, D)
    token_grad = jnp.einsum("bjt,bjd->btd", table_all, row_grad, precision=lax.Precision.HIGHEST)
    token_grad = token_grad.reshape(TOKENS, D).astype(jnp.bfloat16)
    return token_grad, grad_gate, grad_up, grad_down
```

```python
import functools

import jax
import jax.numpy as jnp
from jax import lax
from jax.experimental import pallas as pl
from jax.experimental.pallas import tpu as pltpu
from jax.sharding import PartitionSpec as P

EXPERTS = 8
TOP = 2
F32 = jnp.float32
BF16 = jnp.bfloat16
MESH = pl.DeviceIdType.MESH
NT = (((1,), (1,)), ((), ()))
TN = (((0,), (0,)), ((), ()))


class Sizes:
    def __init__(self, n, e, t, held, width, local, hidden):
        self.n, self.e, self.t, self.held = n, e, t, held
        self.pairs = t // 2
        self.plane = e * self.pairs
        self.groups = n * e
        self.block_rows = held * t
        self.tokens = self.groups * self.block_rows
        self.width = width
        self.slice = width // n
        self.capacity = 5 * self.block_rows * TOP // (4 * EXPERTS)
        self.local = local
        self.rows = self.groups * self.capacity
        self.all_rows = local * self.rows
        self.hidden = hidden
        self.cols = 256 if hidden % 256 == 0 else 128
        self.chunks = hidden // self.cols
        self.unit_rows = self.all_rows // 2
        self.per_unit = local // 2 if local >= 2 else 1
        self.part_rows = self.unit_rows // self.per_unit
        self.units = 2 * self.chunks
        self.down_slots = min(4, self.chunks)


def exchange_kernel(
    s,
    tok, dout, route, wg_hbm, wu_hbm, wd_hbm,
    token_grad, x_out, g_out, res_out,
    xy, routes, xtok, ytok, table, x, g, wg, wu, wd, send, recv_a, recv_b, res, pend, rg, tp, pair_in, sum_a,
    plane_in, sum_b,
    wsem, zs, zr, rs, rr, ps, pr, ds, dr, s1, r1, s2, r2, s3, r3, es, er, fs, fr, hs, hr, osem,
):
    n, W, C, FC = s.n, s.slice, s.chunks, s.cols
    z, e, t = (lax.axis_index(a) for a in ("dp", "expert", "tensor"))
    t2, par = t // 2, t % 2
    spot = e * s.pairs + t2
    group = z * s.e + e

    def remote(src, dst, ssem, rsem, dev):
        return pltpu.make_async_remote_copy(
            src_ref=src, dst_ref=dst, send_sem=ssem, recv_sem=rsem, device_id=dev, device_id_type=MESH
        )

    def plane_dev(q):
        return {"expert": q // s.pairs, "tensor": (q % s.pairs) * 2 + par}

    def group_dev(k):
        return {"dp": k // s.e, "expert": k % s.e}

    other = {"tensor": t2 * 2 + (1 - par)}

    def gate_load(c):
        return pltpu.make_async_copy(
            wg_hbm.at[:, :, pl.ds(c * FC, FC)], wg.at[:, :, pl.ds(c * FC, FC)], wsem.at[0, c])

    def up_load(c):
        return pltpu.make_async_copy(
            wu_hbm.at[:, :, pl.ds(c * FC, FC)], wu.at[:, :, pl.ds(c * FC, FC)], wsem.at[1, c])

    def down_load(c):
        return pltpu.make_async_copy(
            wd_hbm.at[:, pl.ds(c * FC, FC), :], wd.at[lax.rem(c, s.down_slots)], wsem.at[2, c])

    for c in range(C):
        gate_load(c).start()
        up_load(c).start()
        if c < s.down_slots:
            down_load(c).start()

    barrier = pltpu.get_barrier_semaphore()

    def greet(dev):
        pl.semaphore_signal(barrier, inc=1, device_id=dev, device_id_type=MESH)

    def greet_group(k, _):
        greet(group_dev(lax.rem(group + k, s.groups)))
        return 0

    def greet_plane(k, _):
        greet(plane_dev(lax.rem(spot + k, s.plane)))
        return 0

    lax.fori_loop(1, s.groups, greet_group, 0)
    lax.fori_loop(1, s.plane, greet_plane, 0)
    greet(other)
    pl.semaphore_wait(barrier, s.groups - 1 + s.plane - 1 + 1)

    def z_copy(d, i):
        to = lax.rem(z + d, n)
        src = (tok, dout)[i].at[:, pl.ds(pl.multiple_of(to * W, W), W)]
        return remote(src, xy.at[z, e, t2, par, i], zs.at[d, i], zr.at[d, i], {"dp": to})

    def z_arrival(d, i):
        frm = lax.rem(z + n - d, n)
        dst = xy.at[frm, e, t2, par, i]
        return remote(dst, dst, zs.at[d, i], zr.at[d, i], {"dp": lax.rem(z + d, n)})

    for d in range(1, n):
        for i in range(2):
            z_copy(d, i).start()

    def route_copy(k):
        return remote(route, routes.at[k], rs.at[k], rr.at[k], group_dev(lax.rem(group + k, s.groups)))

    def own_copy(k, i):
        src = (tok, dout)[i].at[:, pl.ds(pl.multiple_of(z * W, W), W)]
        return remote(src, xy.at[z, e, t2, par, i], ps.at[0, k, i], pr.at[0, k, i],
                      plane_dev(lax.rem(spot + k, s.plane)))

    def pass_copy(d, k):
        ref = xy.at[lax.rem(z + n - d, n), e, t2, par]
        return remote(ref, ref, ps.at[d, k, 0], pr.at[d, k, 0], plane_dev(lax.rem(spot + k, s.plane)))

    def own_arrival(k, i):
        q = lax.rem(spot + s.plane - k, s.plane)
        ref = xy.at[z, q // s.pairs, lax.rem(q, s.pairs), par, i]
        return remote(ref, ref, ps.at[0, k, i], pr.at[0, k, i], plane_dev(q))

    def pass_arrival(d, k):
        q = lax.rem(spot + s.plane - k, s.plane)
        ref = xy.at[lax.rem(z + n - d, n), q // s.pairs, lax.rem(q, s.pairs), par]
        return remote(ref, ref, ps.at[d, k, 0], pr.at[d, k, 0], plane_dev(q))

    def core_copy(d):
        ref = xy.at[lax.rem(z + n - d, n), :, :, par]
        return remote(ref, ref, ds.at[d], dr.at[d], other)

    def core_arrival(d):
        ref = xy.at[lax.rem(z + n - d, n), :, :, 1 - par]
        return remote(ref, ref, ds.at[d], dr.at[d], other)

    def loop(lo, hi, fn):
        lax.fori_loop(lo, hi, lambda k, c: (fn(k), c)[1], 0)

    def own_send(k):
        own_copy(k, 0).start()
        own_copy(k, 1).start()

    loop(1, s.plane, own_send)
    loop(1, s.groups, lambda k: route_copy(k).start())
    xy[z, e, t2, par, 0] = tok[:, pl.ds(pl.multiple_of(z * W, W), W)]
    xy[z, e, t2, par, 1] = dout[:, pl.ds(pl.multiple_of(z * W, W), W)]
    for d in range(1, n):
        z_arrival(d, 0).wait_recv()
        z_arrival(d, 1).wait_recv()
        loop(1, s.plane, lambda k: pass_copy(d, k).start())

    rg[...] = jnp.zeros_like(rg)

    def own_wait(k):
        own_arrival(k, 0).wait_recv()
        own_arrival(k, 1).wait_recv()

    loop(1, s.plane, own_wait)
    core_copy(0).start()
    for d in range(1, n):
        loop(1, s.plane, lambda k: pass_arrival(d, k).wait_recv())
        core_copy(d).start()
    loop(1, s.groups, lambda k: route_copy(k).wait_recv())
    for d in range(n):
        core_arrival(d).wait_recv()

    def order(i):
        at = (i // s.plane, lax.rem(i, s.plane) // s.pairs, lax.rem(i, s.pairs))
        rows = pl.ds(pl.multiple_of(i * 2 * s.held, 2 * s.held), 2 * s.held)
        for k, ref in enumerate((xtok, ytok)):
            two = [xy[at[0], at[1], at[2], p, k].astype(F32) for p in range(2)]
            ref[rows, :] = jnp.concatenate(two, 0).astype(BF16)

    loop(0, n * s.plane, order)

    total = lax.fori_loop(1, s.groups, lambda k, acc: acc + routes[k], route[...])
    lane = lax.broadcasted_iota(jnp.int32, (1, s.tokens), 1)
    block = (lane // s.block_rows).astype(F32)
    first = (e * s.local).astype(F32)
    targets, probs = [], []
    for k in range(TOP):
        local = total[TOP + k : TOP + k + 1] - first
        slot = total[2 * TOP + k : 2 * TOP + k + 1]
        keep = (slot < s.capacity) & (local >= 0.0) & (local < s.local)
        targets.append(jnp.where(keep, local * s.rows + block * s.capacity + slot, -1.0))
        probs.append(total[k : k + 1])
    step = 80 if s.all_rows % 80 == 0 else 16

    def dispatch(i):
        rows = pl.ds(pl.multiple_of(i * step, step), step)
        place = (lax.broadcasted_iota(jnp.int32, (step, s.tokens), 0) + i * step).astype(F32)
        hit = [place == targets[k] for k in range(TOP)]
        one = jnp.where(hit[0] | hit[1], 1.0, 0.0).astype(BF16)
        table[rows, :] = one
        weight = jnp.where(hit[0], probs[0], 0.0) + jnp.where(hit[1], probs[1], 0.0)
        weight = jnp.sum(weight, axis=1, keepdims=True)
        x[rows, :] = jnp.dot(one, xtok[...], preferred_element_type=F32).astype(BF16)
        g[rows, :] = (weight * jnp.dot(one, ytok[...], preferred_element_type=F32)).astype(BF16)

    loop(0, s.all_rows // step, dispatch)
    x_copy = pltpu.make_async_copy(x, x_out, osem.at[0])
    g_copy = pltpu.make_async_copy(g, g_out, osem.at[1])
    x_copy.start()
    g_copy.start()

    inner = jnp.where(z < n // 2, n // 2 - 1, n // 2)
    is_mid = z == inner
    across = n - 1 - z
    outer = jnp.where(z < n // 2, z - 1, z + 1)

    def unit(u):
        return u // 2, lax.rem(u, 2)

    def part(ref, u):
        c, h = unit(u)
        return ref.at[c, :, pl.ds(pl.multiple_of(h * s.unit_rows, s.unit_rows), s.unit_rows), :]

    def expert_of(h, j):
        return h * s.per_unit + j if s.local >= 2 else 0

    def row_at(h, j):
        return pl.multiple_of(h * s.unit_rows + j * s.part_rows, 16)

    def forward(u, put):
        c, h = unit(u)

        @pl.when(h == 0)
        def _():
            gate_load(c).wait()
            up_load(c).wait()
            down_load(c).wait()

        columns = pl.ds(pl.multiple_of(c * FC, FC), FC)
        for j in range(s.per_unit):
            l = expert_of(h, j)
            rows = pl.ds(row_at(h, j), s.part_rows)
            xs, gs = x[rows, :], g[rows, :]
            put(0, c, h, j, jnp.dot(xs, wg[l, :, columns], preferred_element_type=F32))
            put(1, c, h, j, jnp.dot(xs, wu[l, :, columns], preferred_element_type=F32))
            put(2, c, h, j, lax.dot_general(
                gs, wd[lax.rem(c, s.down_slots), l], NT, preferred_element_type=F32))

        @pl.when((h == 1) & (c + s.down_slots < C))
        def _():
            down_load(c + s.down_slots).start()

    def backward(u):
        c, h = unit(u)
        columns = pl.ds(pl.multiple_of(c * FC, FC), FC)
        for j in range(s.per_unit):
            l = expert_of(h, j)
            rows = pl.ds(row_at(h, j), s.part_rows)
            add = lax.dot_general(res[c, 1, rows, :], wg[l, :, columns], NT, preferred_element_type=F32)
            add = add + lax.dot_general(res[c, 2, rows, :], wu[l, :, columns], NT, preferred_element_type=F32)
            rg[rows, :] += add

    def res_copy(u):
        return pltpu.make_async_copy(part(res, u), part(res_out, u), osem.at[2 + u])

    def to_inner(u):
        return remote(part(send, u), part(recv_a, u), s1.at[u], r1.at[u], {"dp": inner})

    def to_across(u):
        return remote(part(send, u), part(recv_b, u), s2.at[u], r2.at[u], {"dp": across})

    def to_outer(u):
        return remote(part(res, u), part(res, u), s3.at[u], r3.at[u], {"dp": outer})

    @pl.when(jnp.logical_not(is_mid))
    def _():
        def first_half(u):
            def put(i, c, h, j, v):
                send[c, i, pl.ds(row_at(h, j), s.part_rows), :] = v.astype(BF16)

            forward(u, put)
            to_inner(u).start()

        loop(0, s.units, first_half)

        def second_half(u):
            remote(part(res, u), part(res, u), s3.at[u], r3.at[u], {"dp": inner}).wait_recv()
            res_copy(u).start()
            backward(u)

        loop(0, s.units, second_half)
        loop(0, s.units, lambda u: to_inner(u).wait_send())

    @pl.when(is_mid)
    def _():
        tile = 16

        def tiles(fn):
            loop(0, s.unit_rows // tile, lambda i: fn(pl.multiple_of(i * tile, tile)))

        def stage_a(u):
            slot = lax.rem(u, 2)
            c, h = unit(u)

            def put(i, c, h, j, v):
                pend[slot, i, pl.ds(j * s.part_rows, s.part_rows), :] = v

            forward(u, put)
            remote(part(recv_a, u), part(recv_a, u), s1.at[u], r1.at[u], {"dp": outer}).wait_recv()

            def add(r):
                here = pl.ds(r, tile)
                there = pl.ds(pl.multiple_of(h * s.unit_rows + r, tile), tile)
                for i in range(3):
                    v = pend[slot, i, here, :] + recv_a[c, i, there, :].astype(F32)
                    pend[slot, i, here, :] = v
                    send[c, i, there, :] = v.astype(BF16)

            tiles(add)
            to_across(u).start()

        def stage_b(u):
            slot = lax.rem(u, 2)
            c, h = unit(u)
            to_across(u).wait_recv()

            def act(r):
                here = pl.ds(r, tile)
                there = pl.ds(pl.multiple_of(h * s.unit_rows + r, tile), tile)
                pg, pu, gh = (
                    pend[slot, i, here, :] + recv_b[c, i, there, :].astype(F32) for i in range(3)
                )
                sg = jax.nn.sigmoid(pg)
                silu = pg * sg
                res[c, 0, there, :] = (silu * pu).astype(BF16)
                res[c, 1, there, :] = (gh * pu * sg * (1.0 + pg * (1.0 - sg))).astype(BF16)
                res[c, 2, there, :] = (gh * silu).astype(BF16)

            tiles(act)
            to_outer(u).start()
            res_copy(u).start()
            backward(u)

        stage_a(0)

        def both(u):
            stage_a(u)
            stage_b(u - 1)

        loop(1, s.units, both)
        stage_b(s.units - 1)
        loop(0, s.units, lambda u: to_across(u).wait_send())
        loop(0, s.units, lambda u: to_outer(u).wait_send())

    span = 128 if s.tokens % 128 == 0 else s.tokens
    per = span // (2 * s.held)
    rows16 = rg[...].astype(BF16)

    def combine(i):
        lanes = pl.ds(pl.multiple_of(i * span, span), span)
        out = lax.dot_general(table[:, lanes], rows16, TN, preferred_element_type=F32)
        for j in range(per):
            k = i * per + j
            at = (k // s.plane, lax.rem(k, s.plane) // s.pairs, lax.rem(k, s.pairs))
            for p in range(2):
                lo = (2 * j + p) * s.held
                tp[at[0], at[1], at[2], p] = out[lo : lo + s.held].astype(BF16)

    loop(0, s.tokens // span, combine)
    pair_copy = remote(tp.at[:, :, :, 1 - par], pair_in, es, er, other)
    pair_copy.start()
    pair_copy.wait_recv()

    def pair_sum(i):
        at = (i // s.plane, lax.rem(i, s.plane) // s.pairs, lax.rem(i, s.pairs))
        v = tp[at[0], at[1], at[2], par].astype(F32) + pair_in[at].astype(F32)
        sum_a[at] = v.astype(BF16)

    loop(0, n * s.plane, pair_sum)

    def plane_copy(k):
        q = lax.rem(spot + k, s.plane)
        return remote(sum_a.at[:, q // s.pairs, lax.rem(q, s.pairs)], plane_in.at[k], fs.at[k], fr.at[k],
                      plane_dev(q))

    loop(1, s.plane, lambda k: plane_copy(k).start())
    loop(1, s.plane, lambda k: plane_copy(k).wait_recv())

    def last(d):
        to = lax.rem(z + d, n)
        v = sum_a[to, e, t2].astype(F32)
        return to, lax.fori_loop(1, s.plane, lambda k, a: a + plane_in[k, to].astype(F32), v).astype(BF16)

    def final_copy(d):
        to = lax.rem(z + d, n)
        return remote(sum_b.at[to], token_grad.at[:, pl.ds(pl.multiple_of(z * W, W), W)], hs.at[d], hr.at[d],
                      {"dp": to})

    def final_arrival(d):
        frm = lax.rem(z + n - d, n)
        return remote(sum_b.at[frm], token_grad.at[:, pl.ds(pl.multiple_of(frm * W, W), W)], hs.at[d], hr.at[d],
                      {"dp": frm})

    for d in range(1, n):
        to, v = last(d)
        sum_b[to] = v
        final_copy(d).start()
    _, v = last(0)
    token_grad[:, pl.ds(pl.multiple_of(z * W, W), W)] = v

    for d in range(1, n):
        for i in range(2):
            z_copy(d, i).wait_send()
        loop(1, s.plane, lambda k: pass_copy(d, k).wait_send())
        core_copy(d).wait_send()

    def own_sent(k):
        own_copy(k, 0).wait_send()
        own_copy(k, 1).wait_send()

    loop(1, s.plane, own_sent)
    core_copy(0).wait_send()
    loop(1, s.groups, lambda k: route_copy(k).wait_send())
    pair_copy.wait_send()
    loop(1, s.plane, lambda k: plane_copy(k).wait_send())
    x_copy.wait()
    g_copy.wait()
    loop(0, s.units, lambda u: res_copy(u).wait())
    for d in range(1, n):
        final_copy(d).wait_send()
        final_arrival(d).wait_recv()


def exchange(s, tokens, out_grad, route, w_gate, w_up, w_down):
    n, E, T2, M, held, W = s.n, s.e, s.pairs, s.plane, s.held, s.slice
    R, C, FC, L, U = s.all_rows, s.chunks, s.cols, s.local, s.units
    vmem = pl.BlockSpec(memory_space=pltpu.VMEM)
    anywhere = pl.BlockSpec(memory_space=pl.ANY)
    dma = pltpu.SemaphoreType.DMA
    return pl.pallas_call(
        functools.partial(exchange_kernel, s),
        out_shape=(
            jax.ShapeDtypeStruct((held, s.width), BF16),
            jax.ShapeDtypeStruct((R, W), BF16),
            jax.ShapeDtypeStruct((R, W), BF16),
            jax.ShapeDtypeStruct((C, 3, R, FC), BF16),
        ),
        in_specs=[vmem] * 3 + [anywhere] * 3,
        out_specs=(vmem, anywhere, anywhere, anywhere),
        scratch_shapes=[
            pltpu.VMEM((n, E, T2, 2, 2, held, W), BF16),
            pltpu.VMEM((s.groups, 8, s.tokens), F32),
            pltpu.VMEM((s.tokens, W), BF16),
            pltpu.VMEM((s.tokens, W), BF16),
            pltpu.VMEM((R, s.tokens), BF16),
            pltpu.VMEM((R, W), BF16),
            pltpu.VMEM((R, W), BF16),
            pltpu.VMEM((L, W, s.hidden), BF16),
            pltpu.VMEM((L, W, s.hidden), BF16),
            pltpu.VMEM((s.down_slots, L, FC, W), BF16),
            pltpu.VMEM((C, 3, R, FC), BF16),
            pltpu.VMEM((C, 3, R, FC), BF16),
            pltpu.VMEM((C, 3, R, FC), BF16),
            pltpu.VMEM((C, 3, R, FC), BF16),
            pltpu.VMEM((2, 3, s.unit_rows, FC), F32),
            pltpu.VMEM((R, W), F32),
            pltpu.VMEM((n, E, T2, 2, held, W), BF16),
            pltpu.VMEM((n, E, T2, held, W), BF16),
            pltpu.VMEM((n, E, T2, held, W), BF16),
            pltpu.VMEM((M, n, held, W), BF16),
            pltpu.VMEM((n, held, W), BF16),
            dma((3, C)),
            dma((n, 2)), dma((n, 2)),
            dma((s.groups,)), dma((s.groups,)),
            dma((n, M, 2)), dma((n, M, 2)),
            dma((n,)), dma((n,)),
            dma((U,)), dma((U,)), dma((U,)), dma((U,)), dma((U,)), dma((U,)),
            dma, dma,
            dma((M,)), dma((M,)),
            dma((n,)), dma((n,)),
            dma((2 + U,)),
        ],
        compiler_params=pltpu.CompilerParams(
            collective_id=0, has_side_effects=True, vmem_limit_bytes=67_043_328),
        name="exchange",
    )(tokens, out_grad, route, w_gate, w_up, w_down)


def grads_kernel(s, many, x, g, res, gate, up, down):
    for j in range(many):
        rows = pl.ds(j * s.rows, s.rows)
        at = pl.ds(pl.multiple_of((pl.program_id(1) * many + j) * s.rows, 16), s.rows)
        xs, gs = x[at, :], g[at, :]
        gate[j] = lax.dot_general(xs, res[0, 1, rows, :], TN, preferred_element_type=F32).astype(BF16)
        up[j] = lax.dot_general(xs, res[0, 2, rows, :], TN, preferred_element_type=F32).astype(BF16)
        down[j] = lax.dot_general(res[0, 0, rows, :], gs, TN, preferred_element_type=F32).astype(BF16)


def weight_grads(s, x, g, res):
    many = 2 if s.local % 2 == 0 else 1
    W, R, FC = s.slice, s.all_rows, s.cols
    whole = pl.BlockSpec(memory_space=pltpu.VMEM)
    wide = pl.BlockSpec((many, W, FC), lambda c, l: (l, 0, c))
    tall = pl.BlockSpec((many, FC, W), lambda c, l: (l, c, 0))
    return pl.pallas_call(
        functools.partial(grads_kernel, s, many),
        grid=(s.chunks, s.local // many),
        out_shape=(
            jax.ShapeDtypeStruct((s.local, W, s.hidden), BF16),
            jax.ShapeDtypeStruct((s.local, W, s.hidden), BF16),
            jax.ShapeDtypeStruct((s.local, s.hidden, W), BF16),
        ),
        in_specs=[whole, whole, pl.BlockSpec((1, 3, many * s.rows, FC), lambda c, l: (c, 0, l, 0))],
        out_specs=(wide, wide, tall),
        compiler_params=pltpu.CompilerParams(dimension_semantics=("arbitrary", "arbitrary")),
        name="weight_grads",
    )(x, g, res)


def shards(tokens, out_grad, route_probs, expert_ids, slot_index, w_gate, w_up, w_down):
    n, e, t = (lax.axis_size(a) for a in ("dp", "expert", "tensor"))
    held, width = tokens.shape
    s = Sizes(n, e, t, held, width, w_gate.shape[0], w_gate.shape[2])
    own = lax.axis_index("dp") * e + lax.axis_index("expert")
    rows = [route_probs, expert_ids.astype(F32), slot_index.astype(F32)]
    rows = jnp.concatenate(rows + [jnp.zeros((s.block_rows, 8 - 3 * TOP), F32)], axis=1).T
    here = lax.broadcasted_iota(jnp.int32, (8, s.groups, s.block_rows), 1) == own
    route = jnp.where(here, rows[:, None, :], 0.0).reshape(8, s.tokens)
    token_grad, x, g, res = exchange(s, tokens, out_grad, route, w_gate, w_up, w_down)
    gate, up, down = weight_grads(s, x, g, res)
    return token_grad, gate, up, down


def solution(mesh):
    placed = (
        P(("dp", "expert", "tensor"), None),
        P(("dp", "expert", "tensor"), None),
        P(("dp", "expert"), None),
        P(("dp", "expert"), None),
        P(("dp", "expert"), None),
        P("expert", "dp", "tensor"),
        P("expert", "dp", "tensor"),
        P("expert", "tensor", "dp"),
    )
    return jax.shard_map(
        shards,
        mesh=mesh,
        in_specs=placed,
        out_specs=(
            P(("dp", "expert", "tensor"), None),
            P("expert", "dp", "tensor"),
            P("expert", "dp", "tensor"),
            P("expert", "tensor", "dp"),
        ),
        check_vma=False,
    )
```

```python
import functools

import jax
import jax.numpy as jnp
from jax import lax
from jax.experimental import pallas as pl
from jax.experimental.pallas import tpu as pltpu
from jax.sharding import PartitionSpec as P

EXPERTS = 8
TOP = 2
F32 = jnp.float32
BF16 = jnp.bfloat16
MESH = pl.DeviceIdType.MESH
NT = (((1,), (1,)), ((), ()))
TN = (((0,), (0,)), ((), ()))


class Sizes:
    def __init__(self, n, e, t, held, width, local, hidden):
        self.n, self.e, self.t, self.held = n, e, t, held
        self.pairs = t // 2
        self.plane = e * self.pairs
        self.groups = n * e
        self.block_rows = held * t
        self.tokens = self.groups * self.block_rows
        self.width = width
        self.slice = width // n
        self.capacity = 5 * self.block_rows * TOP // (4 * EXPERTS)
        self.local = local
        self.rows = self.groups * self.capacity
        self.all_rows = local * self.rows
        self.hidden = hidden
        self.cols = 256 if hidden % 256 == 0 else 128
        self.chunks = hidden // self.cols
        self.cuts = 4
        self.unit_rows = self.all_rows // self.cuts
        self.per_unit = max(local // self.cuts, 1)
        self.part_rows = self.unit_rows // self.per_unit
        self.units = self.cuts * self.chunks
        self.subs = self.cols // 128
        self.down_slots = min(4, self.chunks)


def exchange_kernel(
    s,
    tok_hbm, dout_hbm, probs_hbm, ids_hbm, slots_hbm, wg_hbm, wu_hbm, wd_hbm,
    token_grad, x_out, g_out, res_out,
    tok, dout, route_probs, expert_ids, slot_index, xy, route, routes, xtok, ytok, table, x, g, wg, wu, wd, send, recv_a, recv_b, res, pend, rg, tp, pair_in, sum_a,
    plane_in, sum_b,
    wsem, zs, zr, rs, rr, ps, pr, ds, dr, s1, r1, r2, s3, es, er, fs, fr, hs, hr, osem, rsem, isem,
):
    n, W, C, FC = s.n, s.slice, s.chunks, s.cols
    z, e, t = (lax.axis_index(a) for a in ("dp", "expert", "tensor"))
    t2, par = t // 2, t % 2
    spot = e * s.pairs + t2
    group = z * s.e + e

    def remote(src, dst, ssem, rsem, dev):
        return pltpu.make_async_remote_copy(
            src_ref=src, dst_ref=dst, send_sem=ssem, recv_sem=rsem, device_id=dev, device_id_type=MESH
        )

    def plane_dev(q):
        return {"expert": q // s.pairs, "tensor": (q % s.pairs) * 2 + par}

    def group_dev(k):
        return {"dp": k // s.e, "expert": k % s.e}

    other = {"tensor": t2 * 2 + (1 - par)}

    barrier = pltpu.get_barrier_semaphore()

    def greet(dev):
        pl.semaphore_signal(barrier, inc=1, device_id=dev, device_id_type=MESH)

    def greet_group(k, _):
        greet(group_dev(lax.rem(group + k, s.groups)))
        return 0

    def greet_plane(k, _):
        greet(plane_dev(lax.rem(spot + k, s.plane)))
        return 0

    lax.fori_loop(1, s.groups, greet_group, 0)
    lax.fori_loop(1, s.plane, greet_plane, 0)
    greet(other)

    small = ((probs_hbm, route_probs), (ids_hbm, expert_ids), (slots_hbm, slot_index), (tok_hbm, tok), (dout_hbm, dout))
    inputs = [pltpu.make_async_copy(a, b, isem.at[i]) for i, (a, b) in enumerate(small)]
    for copy in inputs:
        copy.start()

    def gate_load(c):
        return pltpu.make_async_copy(
            wg_hbm.at[:, :, pl.ds(c * FC, FC)], wg.at[:, :, pl.ds(c * FC, FC)], wsem.at[c])

    def up_load(c):
        return pltpu.make_async_copy(
            wu_hbm.at[:, :, pl.ds(c * FC, FC)], wu.at[:, :, pl.ds(c * FC, FC)], wsem.at[c])

    def down_load(c):
        return pltpu.make_async_copy(
            wd_hbm.at[:, pl.ds(c * FC, FC), :], wd.at[lax.rem(c, s.down_slots)], wsem.at[c])

    for copy in inputs:
        copy.wait()
    for c in range(C):
        gate_load(c).start()
        up_load(c).start()
        if c < s.down_slots:
            down_load(c).start()

    lane = lax.broadcasted_iota(jnp.int32, (TOP, s.tokens), 1)
    mine = lane // s.block_rows == group
    for i, ref in enumerate((route_probs, expert_ids, slot_index)):
        wide = jnp.concatenate([ref[...].astype(F32)] * s.groups, axis=1)
        route[i * TOP : (i + 1) * TOP, :] = jnp.where(mine, wide, 0.0)
    route[3 * TOP :, :] = jnp.zeros((8 - 3 * TOP, s.tokens), F32)

    pl.semaphore_wait(barrier, s.groups - 1 + s.plane - 1 + 1)

    def z_copy(d, i):
        to = lax.rem(z + d, n)
        src = (tok, dout)[i].at[:, pl.ds(pl.multiple_of(to * W, W), W)]
        return remote(src, xy.at[z, e, t2, par, i], zs.at[d], zr.at[d], {"dp": to})

    def z_arrival(d):
        frm = lax.rem(z + n - d, n)
        dst = xy.at[frm, e, t2, par]
        return remote(dst, dst, zs.at[d], zr.at[d], {"dp": lax.rem(z + d, n)})

    for d in range(1, n):
        for i in range(2):
            z_copy(d, i).start()

    def route_copy(k):
        return remote(route, routes.at[k], rs, rr, group_dev(lax.rem(group + k, s.groups)))

    def all_routes():
        ref = routes.at[pl.ds(1, s.groups - 1)]
        return remote(ref, ref, rs, rr, group_dev(lax.rem(group + 1, s.groups)))

    def all_plane(d):
        ref = plane_in.at[pl.ds(1, s.plane - 1), pl.ds(0, 2)]
        return remote(ref, ref, ps.at[d], pr.at[d], plane_dev(lax.rem(spot + 1, s.plane)))

    def own_copy(k, i):
        src = (tok, dout)[i].at[:, pl.ds(pl.multiple_of(z * W, W), W)]
        return remote(src, xy.at[z, e, t2, par, i], ps.at[0], pr.at[0],
                      plane_dev(lax.rem(spot + k, s.plane)))

    def pass_copy(d, k):
        ref = xy.at[lax.rem(z + n - d, n), e, t2, par]
        return remote(ref, ref, ps.at[d], pr.at[d], plane_dev(lax.rem(spot + k, s.plane)))

    def core_copy(d):
        ref = xy.at[lax.rem(z + n - d, n), :, :, par]
        return remote(ref, ref, ds.at[d], dr.at[d], other)

    def core_arrival(d):
        ref = xy.at[lax.rem(z + n - d, n), :, :, 1 - par]
        return remote(ref, ref, ds.at[d], dr.at[d], other)

    def loop(lo, hi, fn):
        lax.fori_loop(lo, hi, lambda k, c: (fn(k), c)[1], 0)

    def own_send(k):
        own_copy(k, 0).start()
        own_copy(k, 1).start()

    loop(1, s.plane, own_send)
    loop(1, s.groups, lambda k: route_copy(k).start())
    xy[z, e, t2, par, 0] = tok[:, pl.ds(pl.multiple_of(z * W, W), W)]
    xy[z, e, t2, par, 1] = dout[:, pl.ds(pl.multiple_of(z * W, W), W)]
    for d in range(1, n):
        z_arrival(d).wait_recv()
        loop(1, s.plane, lambda k: pass_copy(d, k).start())

    rg[...] = jnp.zeros_like(rg)

    for d in range(n):
        all_plane(d).wait_recv()
        core_copy(d).start()
    all_routes().wait_recv()
    for d in range(n):
        core_arrival(d).wait_recv()

    def order(i):
        at = (i // s.plane, lax.rem(i, s.plane) // s.pairs, lax.rem(i, s.pairs))
        rows = pl.ds(pl.multiple_of(i * 2 * s.held, 2 * s.held), 2 * s.held)
        for k, ref in enumerate((xtok, ytok)):
            two = [xy[at[0], at[1], at[2], p, k].astype(F32) for p in range(2)]
            ref[rows, :] = jnp.concatenate(two, 0).astype(BF16)

    loop(0, n * s.plane, order)

    total = lax.fori_loop(1, s.groups, lambda k, acc: acc + routes[k], route[...])
    block = (lax.broadcasted_iota(jnp.int32, (1, s.tokens), 1) // s.block_rows).astype(F32)
    first = (e * s.local).astype(F32)
    targets, probs = [], []
    for k in range(TOP):
        local = total[TOP + k : TOP + k + 1] - first
        slot = total[2 * TOP + k : 2 * TOP + k + 1]
        keep = (slot < s.capacity) & (local >= 0.0) & (local < s.local)
        targets.append(jnp.where(keep, local * s.rows + block * s.capacity + slot, -1.0))
        probs.append(total[k : k + 1])
    step = 80 if s.all_rows % 80 == 0 else 16

    def dispatch(i):
        rows = pl.ds(pl.multiple_of(i * step, step), step)
        place = (lax.broadcasted_iota(jnp.int32, (step, s.tokens), 0) + i * step).astype(F32)
        hit = [place == targets[k] for k in range(TOP)]
        one = jnp.where(hit[0] | hit[1], 1.0, 0.0).astype(BF16)
        table[rows, :] = one
        weight = jnp.where(hit[0], probs[0], 0.0) + jnp.where(hit[1], probs[1], 0.0)
        weight = jnp.sum(weight, axis=1, keepdims=True)
        x[rows, :] = jnp.dot(one, xtok[...], preferred_element_type=F32).astype(BF16)
        g[rows, :] = (weight * jnp.dot(one, ytok[...], preferred_element_type=F32)).astype(BF16)

    loop(0, s.all_rows // step, dispatch)
    x_copy = pltpu.make_async_copy(x, x_out, osem.at[0])
    g_copy = pltpu.make_async_copy(g, g_out, osem.at[1])
    x_copy.start()
    g_copy.start()

    inner = jnp.where(z < n // 2, n // 2 - 1, n // 2)
    is_mid = z == inner
    across = n - 1 - z
    outer = jnp.where(z < n // 2, z - 1, z + 1)

    def unit(u):
        return u // s.cuts, lax.rem(u, s.cuts)

    def part(ref, u):
        c, h = unit(u)
        return ref.at[c, :, pl.ds(pl.multiple_of(h * s.unit_rows, s.unit_rows), s.unit_rows), :]

    def piece(ref, u, b):
        c, h = unit(u)
        rows = pl.ds(pl.multiple_of(h * s.unit_rows, s.unit_rows), s.unit_rows)
        return ref.at[c, :, rows, pl.ds(b * 128, 128)]

    def expert_of(h, j):
        return h * s.per_unit + j if s.local >= s.cuts else h * s.local // s.cuts

    def row_at(h, j):
        return pl.multiple_of(h * s.unit_rows + j * s.part_rows, 16)

    def forward(u, put):
        c, h = unit(u)

        @pl.when(h == 0)
        def _():
            three = wg.at[:, :, pl.ds(0, 3 * FC)]
            pltpu.make_async_copy(three, three, wsem.at[c]).wait()

        columns = pl.ds(pl.multiple_of(c * FC, FC), FC)
        for j in range(s.per_unit):
            l = expert_of(h, j)
            rows = pl.ds(row_at(h, j), s.part_rows)
            xs, gs = x[rows, :], g[rows, :]
            put(0, c, h, j, jnp.dot(xs, wg[l, :, columns], preferred_element_type=F32))
            put(1, c, h, j, jnp.dot(xs, wu[l, :, columns], preferred_element_type=F32))
            put(2, c, h, j, lax.dot_general(
                gs, wd[lax.rem(c, s.down_slots), l], NT, preferred_element_type=F32))

        @pl.when((h == s.cuts - 1) & (c + s.down_slots < C))
        def _():
            down_load(c + s.down_slots).start()

    def backward(u):
        c, h = unit(u)
        columns = pl.ds(pl.multiple_of(c * FC, FC), FC)
        for j in range(s.per_unit):
            l = expert_of(h, j)
            rows = pl.ds(row_at(h, j), s.part_rows)
            add = lax.dot_general(res[c, 1, rows, :], wg[l, :, columns], NT, preferred_element_type=F32)
            add = add + lax.dot_general(res[c, 2, rows, :], wu[l, :, columns], NT, preferred_element_type=F32)
            rg[rows, :] += add

    def res_copy(u):
        return pltpu.make_async_copy(part(res, u), part(res_out, u), rsem)

    def to_inner(u, b):
        return remote(piece(send, u, b), piece(recv_a, u, b), s1, r1.at[u * s.subs + b], {"dp": inner})

    def from_outer(u, b):
        return remote(piece(recv_a, u, b), piece(recv_a, u, b), s1, r1.at[u * s.subs + b], {"dp": outer})

    def to_across(u, b):
        return remote(piece(send, u, b), piece(recv_b, u, b), s1, r2.at[u * s.subs + b], {"dp": across})

    def to_outer(u, b):
        return remote(piece(res, u, b), piece(res, u, b), s3, r1.at[u * s.subs + b], {"dp": outer})

    def from_inner(u, b):
        return remote(piece(res, u, b), piece(res, u, b), s3, r1.at[u * s.subs + b], {"dp": inner})

    @pl.when(jnp.logical_not(is_mid))
    def _():
        def first_half(u):
            def put(i, c, h, j, v):
                send[c, i, pl.ds(row_at(h, j), s.part_rows), :] = v.astype(BF16)

            forward(u, put)
            for b in range(s.subs):
                to_inner(u, b).start()

        loop(0, s.units, first_half)

        def second_half(u):
            for b in range(s.subs):
                from_inner(u, b).wait_recv()
            res_copy(u).start()
            backward(u)

        loop(0, s.units, second_half)
        remote(send, send, s1, r1.at[0], {"dp": inner}).wait_send()

    @pl.when(is_mid)
    def _():
        tile = 16

        def tiles(fn):
            for i in range(s.unit_rows // tile):
                fn(i * tile)

        def ahead(u):
            def put(i, c, h, j, v):
                pend[lax.rem(u, 3), i, pl.ds(j * s.part_rows, s.part_rows), :] = v

            forward(u, put)

        def stage_a(u):
            slot = lax.rem(u, 3)
            c, h = unit(u)

            for b in range(s.subs):
                from_outer(u, b).wait_recv()
                columns = pl.ds(b * 128, 128)

                def add(r):
                    here = pl.ds(r, tile)
                    there = pl.ds(pl.multiple_of(h * s.unit_rows + r, tile), tile)
                    for i in range(3):
                        v = pend[slot, i, here, columns] + recv_a[c, i, there, columns].astype(F32)
                        pend[slot, i, here, columns] = v
                        send[c, i, there, columns] = v.astype(BF16)

                tiles(add)
                to_across(u, b).start()

        def stage_b(u):
            slot = lax.rem(u, 3)
            c, h = unit(u)
            for b in range(s.subs):
                to_across(u, b).wait_recv()
                columns = pl.ds(b * 128, 128)

                def act(r):
                    here = pl.ds(r, tile)
                    there = pl.ds(pl.multiple_of(h * s.unit_rows + r, tile), tile)
                    pg, pu, gh = (
                        pend[slot, i, here, columns] + recv_b[c, i, there, columns].astype(F32) for i in range(3)
                    )
                    sg = jax.nn.sigmoid(pg)
                    silu = pg * sg
                    res[c, 0, there, columns] = (silu * pu).astype(BF16)
                    res[c, 1, there, columns] = (gh * pu * sg * (1.0 + pg * (1.0 - sg))).astype(BF16)
                    res[c, 2, there, columns] = (gh * silu).astype(BF16)

                tiles(act)
                to_outer(u, b).start()
            res_copy(u).start()
            backward(u)

        ahead(0)

        def both(u):
            @pl.when(u < s.units)
            def _():
                stage_a(u)

            @pl.when(u + 1 < s.units)
            def _():
                ahead(u + 1)

            @pl.when(u >= 1)
            def _():
                stage_b(u - 1)

        loop(0, s.units + 1, both)
        remote(send, send, s1, r1.at[0], {"dp": across}).wait_send()
        remote(res, res, s3, r1.at[0], {"dp": outer}).wait_send()

    span = 128 if s.tokens % 128 == 0 else s.tokens
    per = span // (2 * s.held)
    rows16 = rg[...].astype(BF16)

    def combine(i):
        lanes = pl.ds(pl.multiple_of(i * span, span), span)
        out = lax.dot_general(table[:, lanes], rows16, TN, preferred_element_type=F32)
        for j in range(per):
            k = i * per + j
            at = (k // s.plane, lax.rem(k, s.plane) // s.pairs, lax.rem(k, s.pairs))
            for p in range(2):
                lo = (2 * j + p) * s.held
                tp[at[0], at[1], at[2], p] = out[lo : lo + s.held].astype(BF16)

    loop(0, s.tokens // span, combine)
    pair_copy = remote(tp.at[:, :, :, 1 - par], pair_in, es, er, other)
    pair_copy.start()
    pair_copy.wait_recv()

    def pair_sum(i):
        at = (i // s.plane, lax.rem(i, s.plane) // s.pairs, lax.rem(i, s.pairs))
        v = tp[at[0], at[1], at[2], par].astype(F32) + pair_in[at].astype(F32)
        sum_a[at] = v.astype(BF16)

    loop(0, n * s.plane, pair_sum)

    def plane_copy(d, k):
        q, to = lax.rem(spot + k, s.plane), lax.rem(z + d, n)
        return remote(sum_a.at[to, q // s.pairs, lax.rem(q, s.pairs)], plane_in.at[k, to], fs, fr.at[d],
                      plane_dev(q))

    ranks = [n // 2] + [d for d in range(1, n) if d != n // 2] + [0]
    for d in ranks:
        loop(1, s.plane, lambda k: plane_copy(d, k).start())
    all_in = plane_in.at[pl.ds(1, s.plane - 1)]
    sums = remote(all_in, all_in, fs, fr.at[0], plane_dev(lax.rem(spot + 1, s.plane)))

    def last(d):
        to = lax.rem(z + d, n)
        one_in = plane_in.at[pl.ds(1, s.plane - 1), to]
        remote(one_in, one_in, fs, fr.at[d], plane_dev(lax.rem(spot + 1, s.plane))).wait_recv()
        v = sum_a[to, e, t2].astype(F32)
        return to, lax.fori_loop(1, s.plane, lambda k, a: a + plane_in[k, to].astype(F32), v).astype(BF16)

    def final_copy(d):
        to = lax.rem(z + d, n)
        return remote(sum_b.at[to], token_grad.at[:, pl.ds(pl.multiple_of(z * W, W), W)], hs.at[d], hr.at[d],
                      {"dp": to})

    def final_arrival(d):
        frm = lax.rem(z + n - d, n)
        return remote(sum_b.at[frm], token_grad.at[:, pl.ds(pl.multiple_of(frm * W, W), W)], hs.at[d], hr.at[d],
                      {"dp": frm})

    for d in ranks[:-1]:
        to, v = last(d)
        sum_b[to] = v
        final_copy(d).start()
    _, v = last(0)
    sum_b[z] = v
    own_out = pltpu.make_async_copy(
        sum_b.at[z], token_grad.at[:, pl.ds(pl.multiple_of(z * W, W), W)], osem.at[2])
    own_out.start()

    for d in range(n):
        if d > 0:
            z_arrival(d).wait_send()
        all_plane(d).wait_send()
        core_copy(d).wait_send()
    all_routes().wait_send()
    pair_copy.wait_send()
    sums.wait_send()
    x_copy.wait()
    g_copy.wait()
    own_out.wait()
    pltpu.make_async_copy(res, res_out, rsem).wait()
    for d in range(1, n):
        final_copy(d).wait_send()
        final_arrival(d).wait_recv()


def exchange(s, *args):
    n, E, T2, M, held, W = s.n, s.e, s.pairs, s.plane, s.held, s.slice
    R, C, FC, L, U = s.all_rows, s.chunks, s.cols, s.local, s.units
    anywhere = pl.BlockSpec(memory_space=pl.ANY)
    dma = pltpu.SemaphoreType.DMA
    return pl.pallas_call(
        functools.partial(exchange_kernel, s),
        out_shape=(
            jax.ShapeDtypeStruct((held, s.width), BF16),
            jax.ShapeDtypeStruct((R, W), BF16),
            jax.ShapeDtypeStruct((R, W), BF16),
            jax.ShapeDtypeStruct((C, 3, R, FC), BF16),
        ),
        in_specs=[anywhere] * 8,
        out_specs=(anywhere,) * 4,
        scratch_shapes=[
            pltpu.VMEM((held, s.width), BF16),
            pltpu.VMEM((held, s.width), BF16),
            pltpu.VMEM((TOP, s.block_rows), F32),
            pltpu.VMEM((TOP, s.block_rows), jnp.int32),
            pltpu.VMEM((TOP, s.block_rows), jnp.int32),
            pltpu.VMEM((n, E, T2, 2, 2, held, W), BF16),
            pltpu.VMEM((8, s.tokens), F32),
            pltpu.VMEM((s.groups, 8, s.tokens), F32),
            pltpu.VMEM((s.tokens, W), BF16),
            pltpu.VMEM((s.tokens, W), BF16),
            pltpu.VMEM((R, s.tokens), BF16),
            pltpu.VMEM((R, W), BF16),
            pltpu.VMEM((R, W), BF16),
            pltpu.VMEM((L, W, s.hidden), BF16),
            pltpu.VMEM((L, W, s.hidden), BF16),
            pltpu.VMEM((s.down_slots, L, FC, W), BF16),
            pltpu.VMEM((C, 3, R, FC), BF16),
            pltpu.VMEM((C, 3, R, FC), BF16),
            pltpu.VMEM((C, 3, R, FC), BF16),
            pltpu.VMEM((C, 3, R, FC), BF16),
            pltpu.VMEM((3, 3, s.unit_rows, FC), F32),
            pltpu.VMEM((R, W), F32),
            pltpu.VMEM((n, E, T2, 2, held, W), BF16),
            pltpu.VMEM((n, E, T2, held, W), BF16),
            pltpu.VMEM((n, E, T2, held, W), BF16),
            pltpu.VMEM((M, n, held, W), BF16),
            pltpu.VMEM((n, held, W), BF16),
            dma((C,)),
            dma((n,)), dma((n,)),
            dma, dma,
            dma((n,)), dma((n,)),
            dma((n,)), dma((n,)),
            dma, dma((U * s.subs,)), dma((U * s.subs,)), dma,
            dma, dma,
            dma, dma((n,)),
            dma((n,)), dma((n,)),
            dma((3,)), dma, dma((5,)),
        ],
        compiler_params=pltpu.CompilerParams(
            collective_id=0, has_side_effects=True, vmem_limit_bytes=67_043_328),
        name="exchange",
    )(*args)


def grads_kernel(s, tokens_in, x_hbm, g_hbm, res_hbm, tokens_out, gate_hbm, up_hbm, down_hbm,
                 tokens, x, g, res, gate, up, down, xsem, rsem, wsem):
    C, FC = s.chunks, s.cols
    x_load = pltpu.make_async_copy(x_hbm, x, xsem.at[0])
    g_load = pltpu.make_async_copy(g_hbm, g, xsem.at[1])

    def res_load(c):
        return pltpu.make_async_copy(res_hbm.at[c], res.at[c], rsem.at[c])

    x_load.start()
    res_load(0).start()
    g_load.start()
    tokens_load = pltpu.make_async_copy(tokens_in, tokens, xsem.at[2])
    tokens_store = pltpu.make_async_copy(tokens, tokens_out, xsem.at[2])

    def stores(c, slot):
        columns = pl.ds(pl.multiple_of(c * FC, FC), FC)
        return (
            pltpu.make_async_copy(gate.at[slot], gate_hbm.at[:, :, columns], wsem.at[slot, 0]),
            pltpu.make_async_copy(up.at[slot], up_hbm.at[:, :, columns], wsem.at[slot, 1]),
            pltpu.make_async_copy(down.at[slot], down_hbm.at[:, columns, :], wsem.at[slot, 2]),
        )

    x_load.wait()
    for c in range(1, C):
        res_load(c).start()
    tokens_load.start()

    def step(c, carry):
        slot = lax.rem(c, 2)
        out = stores(c, slot)
        res_load(c).wait()
        for i, buffer in ((1, gate), (2, up), (0, down)):
            @pl.when(c >= 2)
            def _():
                out[(i + 2) % 3].wait()

            if i == 0:
                @pl.when(c == 0)
                def _():
                    g_load.wait()

            for l in range(s.local):
                rows = pl.ds(l * s.rows, s.rows)
                left, right = (res[c, 0, rows, :], g[rows, :]) if i == 0 else (x[rows, :], res[c, i, rows, :])
                buffer[slot, l] = lax.dot_general(left, right, TN, preferred_element_type=F32).astype(BF16)
            out[(i + 2) % 3].start()
        return carry

    lax.fori_loop(0, C, step, 0)
    tokens_load.wait()
    tokens_store.start()
    for c in range(max(C - 2, 0), C):
        for copy in stores(c, c % 2):
            copy.wait()
    tokens_store.wait()


def weight_grads(s, token_grad, x, g, res):
    W, FC, R, C, L = s.slice, s.cols, s.all_rows, s.chunks, s.local
    anywhere = pl.BlockSpec(memory_space=pl.ANY)
    dma = pltpu.SemaphoreType.DMA
    return pl.pallas_call(
        functools.partial(grads_kernel, s),
        out_shape=(
            jax.ShapeDtypeStruct((s.held, s.width), BF16),
            jax.ShapeDtypeStruct((L, W, s.hidden), BF16),
            jax.ShapeDtypeStruct((L, W, s.hidden), BF16),
            jax.ShapeDtypeStruct((L, s.hidden, W), BF16),
        ),
        in_specs=[anywhere] * 4,
        out_specs=(anywhere,) * 4,
        scratch_shapes=[
            pltpu.VMEM((s.held, s.width), BF16),
            pltpu.VMEM((R, W), BF16),
            pltpu.VMEM((R, W), BF16),
            pltpu.VMEM((C, 3, R, FC), BF16),
            pltpu.VMEM((2, L, W, FC), BF16),
            pltpu.VMEM((2, L, W, FC), BF16),
            pltpu.VMEM((2, L, FC, W), BF16),
            dma((3,)), dma((C,)), dma((2, 3)),
        ],
        name="weight_grads",
    )(token_grad, x, g, res)


def shards(tokens, out_grad, route_probs, expert_ids, slot_index, w_gate, w_up, w_down):
    n, e, t = (lax.axis_size(a) for a in ("dp", "expert", "tensor"))
    held, width = tokens.shape
    s = Sizes(n, e, t, held, width, w_gate.shape[0], w_gate.shape[2])
    token_grad, x, g, res = exchange(
        s, tokens, out_grad, route_probs.T, expert_ids.T, slot_index.T, w_gate, w_up, w_down)
    return weight_grads(s, token_grad, x, g, res)


def solution(mesh):
    placed = (
        P(("dp", "expert", "tensor"), None),
        P(("dp", "expert", "tensor"), None),
        P(("dp", "expert"), None),
        P(("dp", "expert"), None),
        P(("dp", "expert"), None),
        P("expert", "dp", "tensor"),
        P("expert", "dp", "tensor"),
        P("expert", "tensor", "dp"),
    )
    return jax.shard_map(
        shards,
        mesh=mesh,
        in_specs=placed,
        out_specs=(
            P(("dp", "expert", "tensor"), None),
            P("expert", "dp", "tensor"),
            P("expert", "dp", "tensor"),
            P("expert", "tensor", "dp"),
        ),
        check_vma=False,
    )
```

```python
import functools

import jax
import jax.numpy as jnp
from jax import lax
from jax.experimental import pallas as pl
from jax.experimental.pallas import tpu as pltpu
from jax.sharding import PartitionSpec as P

EXPERTS = 8
TOP = 2
F32 = jnp.float32
BF16 = jnp.bfloat16
MESH = pl.DeviceIdType.MESH
NT = (((1,), (1,)), ((), ()))
TN = (((0,), (0,)), ((), ()))


class Sizes:
    def __init__(self, n, e, t, held, width, local, hidden):
        self.n, self.e, self.t, self.held = n, e, t, held
        self.pairs = t // 2
        self.plane = e * self.pairs
        self.groups = n * e
        self.block_rows = held * t
        self.tokens = self.groups * self.block_rows
        self.width = width
        self.slice = width // n
        self.capacity = 5 * self.block_rows * TOP // (4 * EXPERTS)
        self.local = local
        self.rows = self.groups * self.capacity
        self.all_rows = local * self.rows
        self.hidden = hidden
        self.cols = 256 if hidden % 256 == 0 else 128
        self.chunks = hidden // self.cols
        self.cuts = 4
        self.unit_rows = self.all_rows // self.cuts
        self.per_unit = max(local // self.cuts, 1)
        self.part_rows = self.unit_rows // self.per_unit
        self.units = self.cuts * self.chunks
        self.subs = 1
        self.down_slots = min(4, self.chunks)


def exchange_kernel(
    s,
    tok_hbm, dout_hbm, probs_hbm, ids_hbm, slots_hbm, wg_hbm, wu_hbm, wd_hbm,
    token_grad, x_out, g_out, res_out,
    tok, dout, route_probs, expert_ids, slot_index, xy, route, routes, xtok, ytok, table, x, g, wg, wu, wd, send, recv_a, recv_b, res, pend, rg, tp, pair_in, sum_a,
    plane_in, sum_b,
    wsem, zs, zr, rs, rr, ps, pr, ds, dr, s1, r1, r2, s3, es, er, fs, fr, hs, hr, osem, rsem, isem,
):
    n, W, C, FC = s.n, s.slice, s.chunks, s.cols
    z, e, t = (lax.axis_index(a) for a in ("dp", "expert", "tensor"))
    t2, par = t // 2, t % 2
    spot = e * s.pairs + t2
    group = z * s.e + e

    def remote(src, dst, ssem, rsem, dev):
        return pltpu.make_async_remote_copy(
            src_ref=src, dst_ref=dst, send_sem=ssem, recv_sem=rsem, device_id=dev, device_id_type=MESH
        )

    def plane_dev(q):
        return {"expert": q // s.pairs, "tensor": (q % s.pairs) * 2 + par}

    def group_dev(k):
        return {"dp": k // s.e, "expert": k % s.e}

    other = {"tensor": t2 * 2 + (1 - par)}

    barrier = pltpu.get_barrier_semaphore()

    def greet(dev):
        pl.semaphore_signal(barrier, inc=1, device_id=dev, device_id_type=MESH)

    def greet_group(k, _):
        greet(group_dev(lax.rem(group + k, s.groups)))
        return 0

    def greet_plane(k, _):
        greet(plane_dev(lax.rem(spot + k, s.plane)))
        return 0

    lax.fori_loop(1, s.groups, greet_group, 0)
    lax.fori_loop(1, s.plane, greet_plane, 0)
    greet(other)

    small = ((probs_hbm, route_probs), (ids_hbm, expert_ids), (slots_hbm, slot_index), (tok_hbm, tok), (dout_hbm, dout))
    inputs = [pltpu.make_async_copy(a, b, isem.at[i]) for i, (a, b) in enumerate(small)]
    for copy in inputs:
        copy.start()

    def gate_load(c):
        return pltpu.make_async_copy(
            wg_hbm.at[:, :, pl.ds(c * FC, FC)], wg.at[:, :, pl.ds(c * FC, FC)], wsem.at[c])

    def up_load(c):
        return pltpu.make_async_copy(
            wu_hbm.at[:, :, pl.ds(c * FC, FC)], wu.at[:, :, pl.ds(c * FC, FC)], wsem.at[c])

    def down_load(c):
        return pltpu.make_async_copy(
            wd_hbm.at[:, pl.ds(c * FC, FC), :], wd.at[lax.rem(c, s.down_slots)], wsem.at[c])

    for copy in inputs:
        copy.wait()
    for c in range(C):
        gate_load(c).start()
        up_load(c).start()
        if c < s.down_slots:
            down_load(c).start()

    lane = lax.broadcasted_iota(jnp.int32, (TOP, s.tokens), 1)
    mine = lane // s.block_rows == group
    for i, ref in enumerate((route_probs, expert_ids, slot_index)):
        wide = jnp.concatenate([ref[...].astype(F32)] * s.groups, axis=1)
        route[i * TOP : (i + 1) * TOP, :] = jnp.where(mine, wide, 0.0)
    route[3 * TOP :, :] = jnp.zeros((8 - 3 * TOP, s.tokens), F32)

    pl.semaphore_wait(barrier, s.groups - 1 + s.plane - 1 + 1)

    def z_copy(d, i):
        to = lax.rem(z + d, n)
        src = (tok, dout)[i].at[:, pl.ds(pl.multiple_of(to * W, W), W)]
        return remote(src, xy.at[z, e, t2, par, i], zs.at[d], zr.at[d], {"dp": to})

    def z_arrival(d):
        frm = lax.rem(z + n - d, n)
        dst = xy.at[frm, e, t2, par]
        return remote(dst, dst, zs.at[d], zr.at[d], {"dp": lax.rem(z + d, n)})

    for d in range(1, n):
        for i in range(2):
            z_copy(d, i).start()

    def route_copy(k):
        return remote(route, routes.at[k], rs, rr, group_dev(lax.rem(group + k, s.groups)))

    def all_routes():
        ref = routes.at[pl.ds(1, s.groups - 1)]
        return remote(ref, ref, rs, rr, group_dev(lax.rem(group + 1, s.groups)))

    def all_plane(d):
        ref = plane_in.at[pl.ds(1, s.plane - 1), pl.ds(0, 2)]
        return remote(ref, ref, ps.at[d], pr.at[d], plane_dev(lax.rem(spot + 1, s.plane)))

    def own_copy(k, i):
        src = (tok, dout)[i].at[:, pl.ds(pl.multiple_of(z * W, W), W)]
        return remote(src, xy.at[z, e, t2, par, i], ps.at[0], pr.at[0],
                      plane_dev(lax.rem(spot + k, s.plane)))

    def pass_copy(d, k):
        ref = xy.at[lax.rem(z + n - d, n), e, t2, par]
        return remote(ref, ref, ps.at[d], pr.at[d], plane_dev(lax.rem(spot + k, s.plane)))

    def core_copy(d):
        ref = xy.at[lax.rem(z + n - d, n), :, :, par]
        return remote(ref, ref, ds.at[d], dr.at[d], other)

    def core_arrival(d):
        ref = xy.at[lax.rem(z + n - d, n), :, :, 1 - par]
        return remote(ref, ref, ds.at[d], dr.at[d], other)

    def loop(lo, hi, fn):
        lax.fori_loop(lo, hi, lambda k, c: (fn(k), c)[1], 0)

    def own_send(k):
        own_copy(k, 0).start()
        own_copy(k, 1).start()

    loop(1, s.plane, own_send)
    loop(1, s.groups, lambda k: route_copy(k).start())
    xy[z, e, t2, par, 0] = tok[:, pl.ds(pl.multiple_of(z * W, W), W)]
    xy[z, e, t2, par, 1] = dout[:, pl.ds(pl.multiple_of(z * W, W), W)]
    for d in range(1, n):
        z_arrival(d).wait_recv()
        loop(1, s.plane, lambda k: pass_copy(d, k).start())

    rg[...] = jnp.zeros_like(rg)

    for d in range(n):
        all_plane(d).wait_recv()
        core_copy(d).start()
    all_routes().wait_recv()
    for d in range(n):
        core_arrival(d).wait_recv()

    def order(i):
        at = (i // s.plane, lax.rem(i, s.plane) // s.pairs, lax.rem(i, s.pairs))
        rows = pl.ds(pl.multiple_of(i * 2 * s.held, 2 * s.held), 2 * s.held)
        for k, ref in enumerate((xtok, ytok)):
            two = [xy[at[0], at[1], at[2], p, k].astype(F32) for p in range(2)]
            ref[rows, :] = jnp.concatenate(two, 0).astype(BF16)

    loop(0, n * s.plane, order)

    total = lax.fori_loop(1, s.groups, lambda k, acc: acc + routes[k], route[...])
    block = (lax.broadcasted_iota(jnp.int32, (1, s.tokens), 1) // s.block_rows).astype(F32)
    first = (e * s.local).astype(F32)
    targets, probs = [], []
    for k in range(TOP):
        local = total[TOP + k : TOP + k + 1] - first
        slot = total[2 * TOP + k : 2 * TOP + k + 1]
        keep = (slot < s.capacity) & (local >= 0.0) & (local < s.local)
        targets.append(jnp.where(keep, local * s.rows + block * s.capacity + slot, -1.0))
        probs.append(total[k : k + 1])
    step = 80 if s.all_rows % 80 == 0 else 16

    def dispatch(i):
        rows = pl.ds(pl.multiple_of(i * step, step), step)
        place = (lax.broadcasted_iota(jnp.int32, (step, s.tokens), 0) + i * step).astype(F32)
        hit = [place == targets[k] for k in range(TOP)]
        one = jnp.where(hit[0] | hit[1], 1.0, 0.0).astype(BF16)
        table[rows, :] = one
        weight = jnp.where(hit[0], probs[0], 0.0) + jnp.where(hit[1], probs[1], 0.0)
        weight = jnp.sum(weight, axis=1, keepdims=True)
        x[rows, :] = jnp.dot(one, xtok[...], preferred_element_type=F32).astype(BF16)
        g[rows, :] = (weight * jnp.dot(one, ytok[...], preferred_element_type=F32)).astype(BF16)

    loop(0, s.all_rows // step, dispatch)
    x_copy = pltpu.make_async_copy(x, x_out, osem.at[0])
    g_copy = pltpu.make_async_copy(g, g_out, osem.at[1])
    x_copy.start()
    g_copy.start()

    inner = jnp.where(z < n // 2, n // 2 - 1, n // 2)
    is_mid = z == inner
    across = n - 1 - z
    outer = jnp.where(z < n // 2, z - 1, z + 1)

    def unit(u):
        return u // s.cuts, lax.rem(u, s.cuts)

    def part(ref, u):
        c, h = unit(u)
        return ref.at[c, :, pl.ds(pl.multiple_of(h * s.unit_rows, s.unit_rows), s.unit_rows), :]

    def piece(ref, u, b):
        c, h = unit(u)
        rows = pl.ds(pl.multiple_of(h * s.unit_rows, s.unit_rows), s.unit_rows)
        return ref.at[c, :, rows, pl.ds(0, s.cols)]

    def expert_of(h, j):
        return h * s.per_unit + j if s.local >= s.cuts else h * s.local // s.cuts

    def row_at(h, j):
        return pl.multiple_of(h * s.unit_rows + j * s.part_rows, 16)

    def forward(u, put):
        c, h = unit(u)

        @pl.when(h == 0)
        def _():
            three = wg.at[:, :, pl.ds(0, 3 * FC)]
            pltpu.make_async_copy(three, three, wsem.at[c]).wait()

        columns = pl.ds(pl.multiple_of(c * FC, FC), FC)
        for j in range(s.per_unit):
            l = expert_of(h, j)
            rows = pl.ds(row_at(h, j), s.part_rows)
            xs, gs = x[rows, :], g[rows, :]
            put(0, c, h, j, jnp.dot(xs, wg[l, :, columns], preferred_element_type=F32))
            put(1, c, h, j, jnp.dot(xs, wu[l, :, columns], preferred_element_type=F32))
            put(2, c, h, j, lax.dot_general(
                gs, wd[lax.rem(c, s.down_slots), l], NT, preferred_element_type=F32))

        @pl.when((h == s.cuts - 1) & (c + s.down_slots < C))
        def _():
            down_load(c + s.down_slots).start()

    def backward(u):
        c, h = unit(u)
        columns = pl.ds(pl.multiple_of(c * FC, FC), FC)
        for j in range(s.per_unit):
            l = expert_of(h, j)
            rows = pl.ds(row_at(h, j), s.part_rows)
            add = lax.dot_general(res[c, 1, rows, :], wg[l, :, columns], NT, preferred_element_type=F32)
            add = add + lax.dot_general(res[c, 2, rows, :], wu[l, :, columns], NT, preferred_element_type=F32)
            rg[rows, :] += add

    def res_copy(u):
        return pltpu.make_async_copy(part(res, u), part(res_out, u), rsem)

    def to_inner(u, b):
        return remote(piece(send, u, b), piece(recv_a, u, b), s1, r1.at[u * s.subs + b], {"dp": inner})

    def from_outer(u, b):
        return remote(piece(recv_a, u, b), piece(recv_a, u, b), s1, r1.at[u * s.subs + b], {"dp": outer})

    def to_across(u, b):
        return remote(piece(send, u, b), piece(recv_b, u, b), s1, r2.at[u * s.subs + b], {"dp": across})

    def to_outer(u, b):
        return remote(piece(res, u, b), piece(res, u, b), s3, r1.at[u * s.subs + b], {"dp": outer})

    def from_inner(u, b):
        return remote(piece(res, u, b), piece(res, u, b), s3, r1.at[u * s.subs + b], {"dp": inner})

    @pl.when(jnp.logical_not(is_mid))
    def _():
        def first_half(u):
            def put(i, c, h, j, v):
                send[c, i, pl.ds(row_at(h, j), s.part_rows), :] = v.astype(BF16)

            forward(u, put)
            for b in range(s.subs):
                to_inner(u, b).start()

        loop(0, s.units, first_half)

        def second_half(u):
            for b in range(s.subs):
                from_inner(u, b).wait_recv()
            res_copy(u).start()
            backward(u)

        loop(0, s.units, second_half)
        remote(send, send, s1, r1.at[0], {"dp": inner}).wait_send()

    @pl.when(is_mid)
    def _():
        tile = 16

        def tiles(fn):
            for i in range(s.unit_rows // tile):
                fn(i * tile)

        def ahead(u):
            def put(i, c, h, j, v):
                pend[lax.rem(u, 3), i, pl.ds(j * s.part_rows, s.part_rows), :] = v

            forward(u, put)

        def stage_a(u):
            slot = lax.rem(u, 3)
            c, h = unit(u)

            for b in range(s.subs):
                from_outer(u, b).wait_recv()
                columns = pl.ds(0, s.cols)

                def add(r):
                    here = pl.ds(r, tile)
                    there = pl.ds(pl.multiple_of(h * s.unit_rows + r, tile), tile)
                    for i in range(3):
                        v = pend[slot, i, here, columns] + recv_a[c, i, there, columns].astype(F32)
                        pend[slot, i, here, columns] = v
                        send[c, i, there, columns] = v.astype(BF16)

                tiles(add)
                to_across(u, b).start()

        def stage_b(u):
            slot = lax.rem(u, 3)
            c, h = unit(u)
            for b in range(s.subs):
                to_across(u, b).wait_recv()
                columns = pl.ds(0, s.cols)

                def act(r):
                    here = pl.ds(r, tile)
                    there = pl.ds(pl.multiple_of(h * s.unit_rows + r, tile), tile)
                    pg, pu, gh = (
                        pend[slot, i, here, columns] + recv_b[c, i, there, columns].astype(F32) for i in range(3)
                    )
                    sg = jax.nn.sigmoid(pg)
                    silu = pg * sg
                    res[c, 0, there, columns] = (silu * pu).astype(BF16)
                    res[c, 1, there, columns] = (gh * pu * sg * (1.0 + pg * (1.0 - sg))).astype(BF16)
                    res[c, 2, there, columns] = (gh * silu).astype(BF16)

                tiles(act)
                to_outer(u, b).start()
            res_copy(u).start()
            backward(u)

        ahead(0)

        def both(u):
            @pl.when(u < s.units)
            def _():
                stage_a(u)

            @pl.when(u + 1 < s.units)
            def _():
                ahead(u + 1)

            @pl.when(u >= 1)
            def _():
                stage_b(u - 1)

        loop(0, s.units + 1, both)
        remote(send, send, s1, r1.at[0], {"dp": across}).wait_send()
        remote(res, res, s3, r1.at[0], {"dp": outer}).wait_send()

    span = 128 if s.tokens % 128 == 0 else s.tokens
    per = span // (2 * s.held)
    rows16 = rg[...].astype(BF16)

    def combine(i):
        lanes = pl.ds(pl.multiple_of(i * span, span), span)
        out = lax.dot_general(table[:, lanes], rows16, TN, preferred_element_type=F32)
        for j in range(per):
            k = i * per + j
            at = (k // s.plane, lax.rem(k, s.plane) // s.pairs, lax.rem(k, s.pairs))
            for p in range(2):
                lo = (2 * j + p) * s.held
                tp[at[0], at[1], at[2], p] = out[lo : lo + s.held].astype(BF16)

    def pair_copy(i):
        half = pl.ds(i * (n // 2), n // 2)
        return remote(tp.at[half, :, :, 1 - par], pair_in.at[half], es.at[i], er.at[i], other)

    def pair_sum(i):
        at = (i // s.plane, lax.rem(i, s.plane) // s.pairs, lax.rem(i, s.pairs))
        v = tp[at[0], at[1], at[2], par].astype(F32) + pair_in[at].astype(F32)
        sum_a[at] = v.astype(BF16)

    def plane_copy(to, k):
        q = lax.rem(spot + k, s.plane)
        return remote(sum_a.at[to, q // s.pairs, lax.rem(q, s.pairs)], plane_in.at[k, to], fs, fr.at[to],
                      plane_dev(q))

    spans = s.tokens // span
    for i in range(2):
        loop(i * (spans // 2), (i + 1) * (spans // 2), combine)
        pair_copy(i).start()
    for i in range(2):
        pair_copy(i).wait_recv()
        loop(i * (n * s.plane // 2), (i + 1) * (n * s.plane // 2), pair_sum)
        for to in range(i * (n // 2), (i + 1) * (n // 2)):
            loop(1, s.plane, lambda k: plane_copy(to, k).start())
    all_in = plane_in.at[pl.ds(1, s.plane - 1)]
    sums = remote(all_in, all_in, fs, fr.at[0], plane_dev(lax.rem(spot + 1, s.plane)))

    def last(to):
        one_in = plane_in.at[pl.ds(1, s.plane - 1), to]
        remote(one_in, one_in, fs, fr.at[to], plane_dev(lax.rem(spot + 1, s.plane))).wait_recv()
        v = sum_a[to, e, t2].astype(F32)
        v = lax.fori_loop(1, s.plane, lambda k, a: a + plane_in[k, to].astype(F32), v)
        sum_b[to] = v.astype(BF16)

    def final_copy(d):
        to = lax.rem(z + d, n)
        return remote(sum_b.at[to], token_grad.at[:, pl.ds(pl.multiple_of(z * W, W), W)], hs.at[d], hr.at[d],
                      {"dp": to})

    def final_arrival(d):
        frm = lax.rem(z + n - d, n)
        return remote(sum_b.at[frm], token_grad.at[:, pl.ds(pl.multiple_of(frm * W, W), W)], hs.at[d], hr.at[d],
                      {"dp": frm})

    for to in range(n):
        last(to)

        @pl.when(z != to)
        def _():
            final_copy(lax.rem(to + n - z, n)).start()

    own_out = pltpu.make_async_copy(
        sum_b.at[z], token_grad.at[:, pl.ds(pl.multiple_of(z * W, W), W)], osem.at[2])
    own_out.start()

    for d in range(n):
        if d > 0:
            z_arrival(d).wait_send()
        all_plane(d).wait_send()
        core_copy(d).wait_send()
    all_routes().wait_send()
    for i in range(2):
        pair_copy(i).wait_send()
    sums.wait_send()
    x_copy.wait()
    g_copy.wait()
    own_out.wait()
    pltpu.make_async_copy(res, res_out, rsem).wait()
    for d in range(1, n):
        final_copy(d).wait_send()
        final_arrival(d).wait_recv()


def exchange(s, *args):
    n, E, T2, M, held, W = s.n, s.e, s.pairs, s.plane, s.held, s.slice
    R, C, FC, L, U = s.all_rows, s.chunks, s.cols, s.local, s.units
    anywhere = pl.BlockSpec(memory_space=pl.ANY)
    dma = pltpu.SemaphoreType.DMA
    return pl.pallas_call(
        functools.partial(exchange_kernel, s),
        out_shape=(
            jax.ShapeDtypeStruct((held, s.width), BF16),
            jax.ShapeDtypeStruct((R, W), BF16),
            jax.ShapeDtypeStruct((R, W), BF16),
            jax.ShapeDtypeStruct((C, 3, R, FC), BF16),
        ),
        in_specs=[anywhere] * 8,
        out_specs=(anywhere,) * 4,
        scratch_shapes=[
            pltpu.VMEM((held, s.width), BF16),
            pltpu.VMEM((held, s.width), BF16),
            pltpu.VMEM((TOP, s.block_rows), F32),
            pltpu.VMEM((TOP, s.block_rows), jnp.int32),
            pltpu.VMEM((TOP, s.block_rows), jnp.int32),
            pltpu.VMEM((n, E, T2, 2, 2, held, W), BF16),
            pltpu.VMEM((8, s.tokens), F32),
            pltpu.VMEM((s.groups, 8, s.tokens), F32),
            pltpu.VMEM((s.tokens, W), BF16),
            pltpu.VMEM((s.tokens, W), BF16),
            pltpu.VMEM((R, s.tokens), BF16),
            pltpu.VMEM((R, W), BF16),
            pltpu.VMEM((R, W), BF16),
            pltpu.VMEM((L, W, s.hidden), BF16),
            pltpu.VMEM((L, W, s.hidden), BF16),
            pltpu.VMEM((s.down_slots, L, FC, W), BF16),
            pltpu.VMEM((C, 3, R, FC), BF16),
            pltpu.VMEM((C, 3, R, FC), BF16),
            pltpu.VMEM((C, 3, R, FC), BF16),
            pltpu.VMEM((C, 3, R, FC), BF16),
            pltpu.VMEM((3, 3, s.unit_rows, FC), F32),
            pltpu.VMEM((R, W), F32),
            pltpu.VMEM((n, E, T2, 2, held, W), BF16),
            pltpu.VMEM((n, E, T2, held, W), BF16),
            pltpu.VMEM((n, E, T2, held, W), BF16),
            pltpu.VMEM((M, n, held, W), BF16),
            pltpu.VMEM((n, held, W), BF16),
            dma((C,)),
            dma((n,)), dma((n,)),
            dma, dma,
            dma((n,)), dma((n,)),
            dma((n,)), dma((n,)),
            dma, dma((U * s.subs,)), dma((U * s.subs,)), dma,
            dma((2,)), dma((2,)),
            dma, dma((n,)),
            dma((n,)), dma((n,)),
            dma((3,)), dma, dma((5,)),
        ],
        compiler_params=pltpu.CompilerParams(
            collective_id=0, has_side_effects=True, vmem_limit_bytes=67_043_328),
        name="exchange",
    )(*args)


def grads_kernel(s, tokens_in, x_hbm, g_hbm, res_hbm, tokens_out, gate_hbm, up_hbm, down_hbm,
                 tokens, x, g, res, gate, up, down, xsem, rsem, wsem):
    C, FC = s.chunks, s.cols
    x_load = pltpu.make_async_copy(x_hbm, x, xsem.at[0])
    g_load = pltpu.make_async_copy(g_hbm, g, xsem.at[1])

    def res_load(c):
        return pltpu.make_async_copy(res_hbm.at[c], res.at[c], rsem.at[c])

    x_load.start()
    res_load(0).start()
    g_load.start()
    tokens_load = pltpu.make_async_copy(tokens_in, tokens, xsem.at[2])
    tokens_store = pltpu.make_async_copy(tokens, tokens_out, xsem.at[2])

    def stores(c, slot):
        columns = pl.ds(c * FC, FC)
        return (
            pltpu.make_async_copy(gate.at[slot], gate_hbm.at[:, :, columns], wsem.at[slot, 0]),
            pltpu.make_async_copy(up.at[slot], up_hbm.at[:, :, columns], wsem.at[slot, 1]),
            pltpu.make_async_copy(down.at[slot], down_hbm.at[:, columns, :], wsem.at[slot, 2]),
        )

    x_load.wait()
    for c in range(1, C):
        res_load(c).start()
    tokens_load.start()

    def step(c, carry):
        slot = c % 2
        out = stores(c, slot)
        res_load(c).wait()
        for i, buffer in ((1, gate), (2, up), (0, down)):
            if c >= 2:
                out[(i + 2) % 3].wait()
            if i == 0 and c == 0:
                g_load.wait()

            for l in range(s.local):
                rows = pl.ds(l * s.rows, s.rows)
                left, right = (res[c, 0, rows, :], g[rows, :]) if i == 0 else (x[rows, :], res[c, i, rows, :])
                buffer[slot, l] = lax.dot_general(left, right, TN, preferred_element_type=F32).astype(BF16)
            out[(i + 2) % 3].start()
        return carry

    for c in range(C):
        step(c, 0)
    tokens_load.wait()
    tokens_store.start()
    for c in range(max(C - 2, 0), C):
        for copy in stores(c, c % 2):
            copy.wait()
    tokens_store.wait()


def weight_grads(s, token_grad, x, g, res):
    W, FC, R, C, L = s.slice, s.cols, s.all_rows, s.chunks, s.local
    anywhere = pl.BlockSpec(memory_space=pl.ANY)
    dma = pltpu.SemaphoreType.DMA
    return pl.pallas_call(
        functools.partial(grads_kernel, s),
        out_shape=(
            jax.ShapeDtypeStruct((s.held, s.width), BF16),
            jax.ShapeDtypeStruct((L, W, s.hidden), BF16),
            jax.ShapeDtypeStruct((L, W, s.hidden), BF16),
            jax.ShapeDtypeStruct((L, s.hidden, W), BF16),
        ),
        in_specs=[anywhere] * 4,
        out_specs=(anywhere,) * 4,
        scratch_shapes=[
            pltpu.VMEM((s.held, s.width), BF16),
            pltpu.VMEM((R, W), BF16),
            pltpu.VMEM((R, W), BF16),
            pltpu.VMEM((C, 3, R, FC), BF16),
            pltpu.VMEM((2, L, W, FC), BF16),
            pltpu.VMEM((2, L, W, FC), BF16),
            pltpu.VMEM((2, L, FC, W), BF16),
            dma((3,)), dma((C,)), dma((2, 3)),
        ],
        name="weight_grads",
    )(token_grad, x, g, res)


def shards(tokens, out_grad, route_probs, expert_ids, slot_index, w_gate, w_up, w_down):
    n, e, t = (lax.axis_size(a) for a in ("dp", "expert", "tensor"))
    held, width = tokens.shape
    s = Sizes(n, e, t, held, width, w_gate.shape[0], w_gate.shape[2])
    token_grad, x, g, res = exchange(
        s, tokens, out_grad, route_probs.T, expert_ids.T, slot_index.T, w_gate, w_up, w_down)
    return weight_grads(s, token_grad, x, g, res)


def solution(mesh):
    placed = (
        P(("dp", "expert", "tensor"), None),
        P(("dp", "expert", "tensor"), None),
        P(("dp", "expert"), None),
        P(("dp", "expert"), None),
        P(("dp", "expert"), None),
        P("expert", "dp", "tensor"),
        P("expert", "dp", "tensor"),
        P("expert", "tensor", "dp"),
    )
    return jax.shard_map(
        shards,
        mesh=mesh,
        in_specs=placed,
        out_specs=(
            P(("dp", "expert", "tensor"), None),
            P("expert", "dp", "tensor"),
            P("expert", "dp", "tensor"),
            P("expert", "tensor", "dp"),
        ),
        check_vma=False,
    )
```

```python
import functools

import jax
import jax.numpy as jnp
from jax import lax
from jax.experimental import pallas as pl
from jax.experimental.pallas import tpu as pltpu
from jax.sharding import PartitionSpec as P

EXPERTS = 8
TOP = 2
F32 = jnp.float32
BF16 = jnp.bfloat16
MESH = pl.DeviceIdType.MESH
NT = (((1,), (1,)), ((), ()))
TN = (((0,), (0,)), ((), ()))


class Sizes:
    def __init__(self, n, e, t, held, width, local, hidden):
        self.n, self.e, self.t, self.held = n, e, t, held
        self.pairs = t // 2
        self.plane = e * self.pairs
        self.groups = n * e
        self.block_rows = held * t
        self.tokens = self.groups * self.block_rows
        self.width = width
        self.slice = width // n
        self.capacity = 5 * self.block_rows * TOP // (4 * EXPERTS)
        self.local = local
        self.rows = self.groups * self.capacity
        self.all_rows = local * self.rows
        self.hidden = hidden
        self.cols = 256 if hidden % 256 == 0 else 128
        self.chunks = hidden // self.cols
        self.cuts = 4
        self.unit_rows = self.all_rows // self.cuts
        self.per_unit = max(local // self.cuts, 1)
        self.part_rows = self.unit_rows // self.per_unit
        self.units = self.cuts * self.chunks
        self.subs = 1
        self.down_slots = min(4, self.chunks)


def exchange_kernel(
    s,
    tok_hbm, dout_hbm, probs_hbm, ids_hbm, slots_hbm, wg_hbm, wu_hbm, wd_hbm,
    token_grad, x_out, g_out, res_out,
    tok, dout, route_probs, expert_ids, slot_index, xy, route, routes, xtok, ytok, table, x, g, wg, wu, wd, send, recv_a, recv_b, res, pend, rg, tp, pair_in, sum_a,
    plane_in, sum_b,
    wsem, zs, zr, rs, rr, ps, pr, ds, dr, s1, r1, r2, s3, es, er, fs, fr, hs, hr, osem, rsem, isem,
):
    n, W, C, FC = s.n, s.slice, s.chunks, s.cols
    z, e, t = (lax.axis_index(a) for a in ("dp", "expert", "tensor"))
    t2, par = t // 2, t % 2
    spot = e * s.pairs + t2
    group = z * s.e + e

    def remote(src, dst, ssem, rsem, dev):
        return pltpu.make_async_remote_copy(
            src_ref=src, dst_ref=dst, send_sem=ssem, recv_sem=rsem, device_id=dev, device_id_type=MESH
        )

    def plane_dev(q):
        return {"expert": q // s.pairs, "tensor": (q % s.pairs) * 2 + par}

    def group_dev(k):
        return {"dp": k // s.e, "expert": k % s.e}

    other = {"tensor": t2 * 2 + (1 - par)}

    barrier = pltpu.get_barrier_semaphore()

    def greet(dev):
        pl.semaphore_signal(barrier, inc=1, device_id=dev, device_id_type=MESH)

    def greet_group(k, _):
        greet(group_dev(lax.rem(group + k, s.groups)))
        return 0

    def greet_plane(k, _):
        greet(plane_dev(lax.rem(spot + k, s.plane)))
        return 0

    lax.fori_loop(1, s.groups, greet_group, 0)
    lax.fori_loop(1, s.plane, greet_plane, 0)
    greet(other)

    small = ((probs_hbm, route_probs), (ids_hbm, expert_ids), (slots_hbm, slot_index), (tok_hbm, tok), (dout_hbm, dout))
    inputs = [pltpu.make_async_copy(a, b, isem.at[i]) for i, (a, b) in enumerate(small)]
    for copy in inputs:
        copy.start()

    def gate_load(c):
        return pltpu.make_async_copy(
            wg_hbm.at[:, :, pl.ds(c * FC, FC)], wg.at[:, :, pl.ds(c * FC, FC)], wsem.at[c])

    def up_load(c):
        return pltpu.make_async_copy(
            wu_hbm.at[:, :, pl.ds(c * FC, FC)], wu.at[:, :, pl.ds(c * FC, FC)], wsem.at[c])

    def down_load(c):
        return pltpu.make_async_copy(
            wd_hbm.at[:, pl.ds(c * FC, FC), :], wd.at[lax.rem(c, s.down_slots)], wsem.at[c])

    for copy in inputs:
        copy.wait()
    for c in range(C):
        gate_load(c).start()
        up_load(c).start()
        if c < s.down_slots:
            down_load(c).start()

    lane = lax.broadcasted_iota(jnp.int32, (TOP, s.tokens), 1)
    mine = lane // s.block_rows == group
    for i, ref in enumerate((route_probs, expert_ids, slot_index)):
        wide = jnp.concatenate([ref[...].astype(F32)] * s.groups, axis=1)
        route[i * TOP : (i + 1) * TOP, :] = jnp.where(mine, wide, 0.0)
    route[3 * TOP :, :] = jnp.zeros((8 - 3 * TOP, s.tokens), F32)

    pl.semaphore_wait(barrier, s.groups - 1 + s.plane - 1 + 1)

    def z_copy(d, i):
        to = lax.rem(z + d, n)
        src = (tok, dout)[i].at[:, pl.ds(pl.multiple_of(to * W, W), W)]
        return remote(src, xy.at[z, e, t2, par, i], zs.at[d], zr.at[d], {"dp": to})

    def z_arrival(d):
        frm = lax.rem(z + n - d, n)
        dst = xy.at[frm, e, t2, par]
        return remote(dst, dst, zs.at[d], zr.at[d], {"dp": lax.rem(z + d, n)})

    for d in range(1, n):
        for i in range(2):
            z_copy(d, i).start()

    def route_copy(k):
        return remote(route, routes.at[k], rs, rr, group_dev(lax.rem(group + k, s.groups)))

    def all_routes():
        ref = routes.at[pl.ds(1, s.groups - 1)]
        return remote(ref, ref, rs, rr, group_dev(lax.rem(group + 1, s.groups)))

    def all_plane(d):
        ref = plane_in.at[pl.ds(1, s.plane - 1), pl.ds(0, 2)]
        return remote(ref, ref, ps.at[d], pr.at[d], plane_dev(lax.rem(spot + 1, s.plane)))

    def own_copy(k, i):
        src = (tok, dout)[i].at[:, pl.ds(pl.multiple_of(z * W, W), W)]
        return remote(src, xy.at[z, e, t2, par, i], ps.at[0], pr.at[0],
                      plane_dev(lax.rem(spot + k, s.plane)))

    def pass_copy(d, k):
        ref = xy.at[lax.rem(z + n - d, n), e, t2, par]
        return remote(ref, ref, ps.at[d], pr.at[d], plane_dev(lax.rem(spot + k, s.plane)))

    def core_copy(d):
        ref = xy.at[lax.rem(z + n - d, n), :, :, par]
        return remote(ref, ref, ds.at[d], dr.at[d], other)

    def core_arrival(d):
        ref = xy.at[lax.rem(z + n - d, n), :, :, 1 - par]
        return remote(ref, ref, ds.at[d], dr.at[d], other)

    def loop(lo, hi, fn):
        lax.fori_loop(lo, hi, lambda k, c: (fn(k), c)[1], 0)

    def own_send(k):
        own_copy(k, 0).start()
        own_copy(k, 1).start()

    loop(1, s.plane, own_send)
    loop(1, s.groups, lambda k: route_copy(k).start())
    xy[z, e, t2, par, 0] = tok[:, pl.ds(pl.multiple_of(z * W, W), W)]
    xy[z, e, t2, par, 1] = dout[:, pl.ds(pl.multiple_of(z * W, W), W)]
    for d in range(1, n):
        z_arrival(d).wait_recv()
        loop(1, s.plane, lambda k: pass_copy(d, k).start())

    rg[...] = jnp.zeros_like(rg)

    for d in range(n):
        all_plane(d).wait_recv()
        core_copy(d).start()
    all_routes().wait_recv()
    for d in range(n):
        core_arrival(d).wait_recv()

    def order(i):
        at = (i // s.plane, lax.rem(i, s.plane) // s.pairs, lax.rem(i, s.pairs))
        rows = pl.ds(pl.multiple_of(i * 2 * s.held, 2 * s.held), 2 * s.held)
        for k, ref in enumerate((xtok, ytok)):
            two = [xy[at[0], at[1], at[2], p, k].astype(F32) for p in range(2)]
            ref[rows, :] = jnp.concatenate(two, 0).astype(BF16)

    loop(0, n * s.plane, order)

    total = lax.fori_loop(1, s.groups, lambda k, acc: acc + routes[k], route[...])
    block = (lax.broadcasted_iota(jnp.int32, (1, s.tokens), 1) // s.block_rows).astype(F32)
    first = (e * s.local).astype(F32)
    targets, probs = [], []
    for k in range(TOP):
        local = total[TOP + k : TOP + k + 1] - first
        slot = total[2 * TOP + k : 2 * TOP + k + 1]
        keep = (slot < s.capacity) & (local >= 0.0) & (local < s.local)
        targets.append(jnp.where(keep, local * s.rows + block * s.capacity + slot, -1.0))
        probs.append(total[k : k + 1])
    step = 80 if s.all_rows % 80 == 0 else 16

    def dispatch(i):
        rows = pl.ds(pl.multiple_of(i * step, step), step)
        place = (lax.broadcasted_iota(jnp.int32, (step, s.tokens), 0) + i * step).astype(F32)
        hit = [place == targets[k] for k in range(TOP)]
        one = jnp.where(hit[0] | hit[1], 1.0, 0.0).astype(BF16)
        table[rows, :] = one
        weight = jnp.where(hit[0], probs[0], 0.0) + jnp.where(hit[1], probs[1], 0.0)
        weight = jnp.sum(weight, axis=1, keepdims=True)
        x[rows, :] = jnp.dot(one, xtok[...], preferred_element_type=F32).astype(BF16)
        g[rows, :] = (weight * jnp.dot(one, ytok[...], preferred_element_type=F32)).astype(BF16)

    loop(0, s.all_rows // step, dispatch)
    x_copy = pltpu.make_async_copy(x, x_out, osem.at[0])
    g_copy = pltpu.make_async_copy(g, g_out, osem.at[1])
    x_copy.start()
    g_copy.start()

    inner = jnp.where(z < n // 2, n // 2 - 1, n // 2)
    is_mid = z == inner
    across = n - 1 - z
    outer = jnp.where(z < n // 2, z - 1, z + 1)

    def unit(u):
        return u // s.cuts, lax.rem(u, s.cuts)

    def part(ref, u):
        c, h = unit(u)
        return ref.at[c, :, pl.ds(pl.multiple_of(h * s.unit_rows, s.unit_rows), s.unit_rows), :]

    def piece(ref, u, b):
        c, h = unit(u)
        rows = pl.ds(pl.multiple_of(h * s.unit_rows, s.unit_rows), s.unit_rows)
        return ref.at[c, :, rows, pl.ds(0, s.cols)]

    def expert_of(h, j):
        return h * s.per_unit + j if s.local >= s.cuts else h * s.local // s.cuts

    def row_at(h, j):
        return pl.multiple_of(h * s.unit_rows + j * s.part_rows, 16)

    def forward(u, put):
        c, h = unit(u)

        @pl.when(h == 0)
        def _():
            three = wg.at[:, :, pl.ds(0, 3 * FC)]
            pltpu.make_async_copy(three, three, wsem.at[c]).wait()

        columns = pl.ds(pl.multiple_of(c * FC, FC), FC)
        for j in range(s.per_unit):
            l = expert_of(h, j)
            rows = pl.ds(row_at(h, j), s.part_rows)
            xs, gs = x[rows, :], g[rows, :]
            put(0, c, h, j, jnp.dot(xs, wg[l, :, columns], preferred_element_type=F32))
            put(1, c, h, j, jnp.dot(xs, wu[l, :, columns], preferred_element_type=F32))
            put(2, c, h, j, lax.dot_general(
                gs, wd[lax.rem(c, s.down_slots), l], NT, preferred_element_type=F32))

        @pl.when((h == s.cuts - 1) & (c + s.down_slots < C))
        def _():
            down_load(c + s.down_slots).start()

    def backward(u):
        c, h = unit(u)
        columns = pl.ds(pl.multiple_of(c * FC, FC), FC)
        for j in range(s.per_unit):
            l = expert_of(h, j)
            rows = pl.ds(row_at(h, j), s.part_rows)
            add = lax.dot_general(res[c, 1, rows, :], wg[l, :, columns], NT, preferred_element_type=F32)
            add = add + lax.dot_general(res[c, 2, rows, :], wu[l, :, columns], NT, preferred_element_type=F32)
            rg[rows, :] += add

    def res_copy(u):
        return pltpu.make_async_copy(part(res, u), part(res_out, u), rsem)

    def to_inner(u, b):
        return remote(piece(send, u, b), piece(recv_a, u, b), s1, r1.at[u * s.subs + b], {"dp": inner})

    def from_outer(u, b):
        return remote(piece(recv_a, u, b), piece(recv_a, u, b), s1, r1.at[u * s.subs + b], {"dp": outer})

    def to_across(u, b):
        return remote(piece(send, u, b), piece(recv_b, u, b), s1, r2.at[u * s.subs + b], {"dp": across})

    def to_outer(u, b):
        return remote(piece(res, u, b), piece(res, u, b), s3, r1.at[u * s.subs + b], {"dp": outer})

    def from_inner(u, b):
        return remote(piece(res, u, b), piece(res, u, b), s3, r1.at[u * s.subs + b], {"dp": inner})

    @pl.when(jnp.logical_not(is_mid))
    def _():
        def first_half(u):
            def put(i, c, h, j, v):
                send[c, i, pl.ds(row_at(h, j), s.part_rows), :] = v.astype(BF16)

            forward(u, put)
            for b in range(s.subs):
                to_inner(u, b).start()

        loop(0, s.units, first_half)

        def second_half(u):
            for b in range(s.subs):
                from_inner(u, b).wait_recv()
            res_copy(u).start()
            backward(u)

        loop(0, s.units, second_half)
        remote(send, send, s1, r1.at[0], {"dp": inner}).wait_send()

    @pl.when(is_mid)
    def _():
        tile = 16

        def tiles(fn):
            for i in range(s.unit_rows // tile):
                fn(i * tile)

        def ahead(u):
            def put(i, c, h, j, v):
                pend[lax.rem(u, 3), i, pl.ds(j * s.part_rows, s.part_rows), :] = v

            forward(u, put)

        def stage_a(u):
            slot = lax.rem(u, 3)
            c, h = unit(u)

            for b in range(s.subs):
                from_outer(u, b).wait_recv()
                columns = pl.ds(0, s.cols)

                def add(r):
                    here = pl.ds(r, tile)
                    there = pl.ds(pl.multiple_of(h * s.unit_rows + r, tile), tile)
                    for i in range(3):
                        v = pend[slot, i, here, columns] + recv_a[c, i, there, columns].astype(F32)
                        pend[slot, i, here, columns] = v
                        send[c, i, there, columns] = v.astype(BF16)

                tiles(add)
                to_across(u, b).start()

        def stage_b(u):
            slot = lax.rem(u, 3)
            c, h = unit(u)
            for b in range(s.subs):
                to_across(u, b).wait_recv()
                columns = pl.ds(0, s.cols)

                def act(r):
                    here = pl.ds(r, tile)
                    there = pl.ds(pl.multiple_of(h * s.unit_rows + r, tile), tile)
                    pg, pu, gh = (
                        pend[slot, i, here, columns] + recv_b[c, i, there, columns].astype(F32) for i in range(3)
                    )
                    sg = jax.nn.sigmoid(pg)
                    silu = pg * sg
                    res[c, 0, there, columns] = (silu * pu).astype(BF16)
                    res[c, 1, there, columns] = (gh * pu * sg * (1.0 + pg * (1.0 - sg))).astype(BF16)
                    res[c, 2, there, columns] = (gh * silu).astype(BF16)

                tiles(act)
                to_outer(u, b).start()
            res_copy(u).start()
            backward(u)

        ahead(0)

        def both(u):
            @pl.when(u < s.units)
            def _():
                stage_a(u)

            @pl.when(u + 1 < s.units)
            def _():
                ahead(u + 1)

            @pl.when(u >= 1)
            def _():
                stage_b(u - 1)

        loop(0, s.units + 1, both)
        remote(send, send, s1, r1.at[0], {"dp": across}).wait_send()
        remote(res, res, s3, r1.at[0], {"dp": outer}).wait_send()

    span = 128 if s.tokens % 128 == 0 else s.tokens
    per = span // (2 * s.held)
    rows16 = rg[...].astype(BF16)

    def combine(i):
        lanes = pl.ds(pl.multiple_of(i * span, span), span)
        out = lax.dot_general(table[:, lanes], rows16, TN, preferred_element_type=F32)
        for j in range(per):
            k = i * per + j
            at = (k // s.plane, lax.rem(k, s.plane) // s.pairs, lax.rem(k, s.pairs))
            for p in range(2):
                lo = (2 * j + p) * s.held
                tp[at[0], at[1], at[2], p] = out[lo : lo + s.held].astype(BF16)

    def pair_copy(i):
        half = pl.ds(i * (n // 2), n // 2)
        return remote(tp.at[half, :, :, 1 - par], pair_in.at[half], es.at[i], er.at[i], other)

    def pair_sum(i):
        at = (i // s.plane, lax.rem(i, s.plane) // s.pairs, lax.rem(i, s.pairs))
        v = tp[at[0], at[1], at[2], par].astype(F32) + pair_in[at].astype(F32)
        sum_a[at] = v.astype(BF16)

    def plane_copy(to, k):
        q = lax.rem(spot + k, s.plane)
        return remote(sum_a.at[to, q // s.pairs, lax.rem(q, s.pairs)], plane_in.at[k, to], fs, fr.at[to],
                      plane_dev(q))

    spans = s.tokens // span
    for i in range(2):
        loop(i * (spans // 2), (i + 1) * (spans // 2), combine)
        pair_copy(i).start()
    for i in range(2):
        pair_copy(i).wait_recv()
        loop(i * (n * s.plane // 2), (i + 1) * (n * s.plane // 2), pair_sum)
        for to in range(i * (n // 2), (i + 1) * (n // 2)):
            loop(1, s.plane, lambda k: plane_copy(to, k).start())
    all_in = plane_in.at[pl.ds(1, s.plane - 1)]
    sums = remote(all_in, all_in, fs, fr.at[0], plane_dev(lax.rem(spot + 1, s.plane)))

    def last(to):
        one_in = plane_in.at[pl.ds(1, s.plane - 1), to]
        remote(one_in, one_in, fs, fr.at[to], plane_dev(lax.rem(spot + 1, s.plane))).wait_recv()
        v = sum_a[to, e, t2].astype(F32)
        v = lax.fori_loop(1, s.plane, lambda k, a: a + plane_in[k, to].astype(F32), v)
        sum_b[to] = v.astype(BF16)

    def final_copy(d):
        to = lax.rem(z + d, n)
        return remote(sum_b.at[to], token_grad.at[:, pl.ds(pl.multiple_of(z * W, W), W)], hs.at[d], hr.at[d],
                      {"dp": to})

    def final_arrival(d):
        frm = lax.rem(z + n - d, n)
        return remote(sum_b.at[frm], token_grad.at[:, pl.ds(pl.multiple_of(frm * W, W), W)], hs.at[d], hr.at[d],
                      {"dp": frm})

    for to in range(n):
        last(to)

        @pl.when(z != to)
        def _():
            final_copy(lax.rem(to + n - z, n)).start()

    own_out = pltpu.make_async_copy(
        sum_b.at[z], token_grad.at[:, pl.ds(pl.multiple_of(z * W, W), W)], osem.at[2])
    own_out.start()

    for d in range(n):
        if d > 0:
            z_arrival(d).wait_send()
        all_plane(d).wait_send()
        core_copy(d).wait_send()
    all_routes().wait_send()
    for i in range(2):
        pair_copy(i).wait_send()
    sums.wait_send()
    x_copy.wait()
    g_copy.wait()
    own_out.wait()
    pltpu.make_async_copy(res, res_out, rsem).wait()
    for d in range(1, n):
        final_copy(d).wait_send()
        final_arrival(d).wait_recv()


def exchange(s, *args):
    n, E, T2, M, held, W = s.n, s.e, s.pairs, s.plane, s.held, s.slice
    R, C, FC, L, U = s.all_rows, s.chunks, s.cols, s.local, s.units
    anywhere = pl.BlockSpec(memory_space=pl.ANY)
    dma = pltpu.SemaphoreType.DMA
    return pl.pallas_call(
        functools.partial(exchange_kernel, s),
        out_shape=(
            jax.ShapeDtypeStruct((held, s.width), BF16),
            jax.ShapeDtypeStruct((R, W), BF16),
            jax.ShapeDtypeStruct((R, W), BF16),
            jax.ShapeDtypeStruct((C, 3, R, FC), BF16),
        ),
        in_specs=[anywhere] * 8,
        out_specs=(anywhere,) * 4,
        scratch_shapes=[
            pltpu.VMEM((held, s.width), BF16),
            pltpu.VMEM((held, s.width), BF16),
            pltpu.VMEM((TOP, s.block_rows), F32),
            pltpu.VMEM((TOP, s.block_rows), jnp.int32),
            pltpu.VMEM((TOP, s.block_rows), jnp.int32),
            pltpu.VMEM((n, E, T2, 2, 2, held, W), BF16),
            pltpu.VMEM((8, s.tokens), F32),
            pltpu.VMEM((s.groups, 8, s.tokens), F32),
            pltpu.VMEM((s.tokens, W), BF16),
            pltpu.VMEM((s.tokens, W), BF16),
            pltpu.VMEM((R, s.tokens), BF16),
            pltpu.VMEM((R, W), BF16),
            pltpu.VMEM((R, W), BF16),
            pltpu.VMEM((L, W, s.hidden), BF16),
            pltpu.VMEM((L, W, s.hidden), BF16),
            pltpu.VMEM((s.down_slots, L, FC, W), BF16),
            pltpu.VMEM((C, 3, R, FC), BF16),
            pltpu.VMEM((C, 3, R, FC), BF16),
            pltpu.VMEM((C, 3, R, FC), BF16),
            pltpu.VMEM((C, 3, R, FC), BF16),
            pltpu.VMEM((3, 3, s.unit_rows, FC), F32),
            pltpu.VMEM((R, W), F32),
            pltpu.VMEM((n, E, T2, 2, held, W), BF16),
            pltpu.VMEM((n, E, T2, held, W), BF16),
            pltpu.VMEM((n, E, T2, held, W), BF16),
            pltpu.VMEM((M, n, held, W), BF16),
            pltpu.VMEM((n, held, W), BF16),
            dma((C,)),
            dma((n,)), dma((n,)),
            dma, dma,
            dma((n,)), dma((n,)),
            dma((n,)), dma((n,)),
            dma, dma((U * s.subs,)), dma((U * s.subs,)), dma,
            dma((2,)), dma((2,)),
            dma, dma((n,)),
            dma((n,)), dma((n,)),
            dma((3,)), dma, dma((5,)),
        ],
        compiler_params=pltpu.CompilerParams(
            collective_id=0, has_side_effects=True, vmem_limit_bytes=67_043_328),
        name="exchange",
    )(*args)


def grads_kernel(s, tokens_in, x_hbm, g_hbm, res_hbm, tokens_out, gate_hbm, up_hbm, down_hbm,
                 tokens, x, g, res, gate, up, down, xsem, rsem, wsem):
    C, FC = s.chunks, s.cols
    x_load = pltpu.make_async_copy(x_hbm, x, xsem.at[0])
    g_load = pltpu.make_async_copy(g_hbm, g, xsem.at[1])

    def res_load(c):
        return pltpu.make_async_copy(res_hbm.at[c], res.at[c], rsem.at[c])

    x_load.start()
    res_load(0).start()
    g_load.start()
    tokens_load = pltpu.make_async_copy(tokens_in, tokens, xsem.at[2])
    tokens_store = pltpu.make_async_copy(tokens, tokens_out, xsem.at[2])

    def stores(c, slot):
        columns = pl.ds(c * FC, FC)
        return (
            pltpu.make_async_copy(gate.at[slot], gate_hbm.at[:, :, columns], wsem.at[slot, 0]),
            pltpu.make_async_copy(up.at[slot], up_hbm.at[:, :, columns], wsem.at[slot, 1]),
            pltpu.make_async_copy(down.at[slot], down_hbm.at[:, columns, :], wsem.at[slot, 2]),
        )

    def one_store(i, c, slot, l):
        columns = pl.ds(c * FC, FC)
        if i == 0:
            return pltpu.make_async_copy(down.at[slot, l], down_hbm.at[l, columns, :], wsem.at[slot, 2])
        a, b = ((gate, gate_hbm), (up, up_hbm))[i - 1]
        return pltpu.make_async_copy(a.at[slot, l], b.at[l, :, columns], wsem.at[slot, i - 1])

    x_load.wait()
    for c in range(1, C):
        res_load(c).start()
    tokens_load.start()

    def step(c, carry):
        slot = c % 2
        out = stores(c, slot)
        res_load(c).wait()
        for i, buffer in ((1, gate), (2, up), (0, down)):
            if c >= 2:
                out[(i + 2) % 3].wait()
            if i == 0 and c == 0:
                g_load.wait()

            for l in range(s.local):
                rows = pl.ds(l * s.rows, s.rows)
                left, right = (res[c, 0, rows, :], g[rows, :]) if i == 0 else (x[rows, :], res[c, i, rows, :])
                buffer[slot, l] = lax.dot_general(left, right, TN, preferred_element_type=F32).astype(BF16)
                if c == 0 or c == C - 1:
                    one_store(i, c, slot, l).start()
            if c != 0 and c != C - 1:
                out[(i + 2) % 3].start()
        return carry

    for c in range(C):
        step(c, 0)
    tokens_load.wait()
    tokens_store.start()
    for c in range(max(C - 2, 0), C):
        for copy in stores(c, c % 2):
            copy.wait()
    tokens_store.wait()


def weight_grads(s, token_grad, x, g, res):
    W, FC, R, C, L = s.slice, s.cols, s.all_rows, s.chunks, s.local
    anywhere = pl.BlockSpec(memory_space=pl.ANY)
    dma = pltpu.SemaphoreType.DMA
    return pl.pallas_call(
        functools.partial(grads_kernel, s),
        out_shape=(
            jax.ShapeDtypeStruct((s.held, s.width), BF16),
            jax.ShapeDtypeStruct((L, W, s.hidden), BF16),
            jax.ShapeDtypeStruct((L, W, s.hidden), BF16),
            jax.ShapeDtypeStruct((L, s.hidden, W), BF16),
        ),
        in_specs=[anywhere] * 4,
        out_specs=(anywhere,) * 4,
        scratch_shapes=[
            pltpu.VMEM((s.held, s.width), BF16),
            pltpu.VMEM((R, W), BF16),
            pltpu.VMEM((R, W), BF16),
            pltpu.VMEM((C, 3, R, FC), BF16),
            pltpu.VMEM((2, L, W, FC), BF16),
            pltpu.VMEM((2, L, W, FC), BF16),
            pltpu.VMEM((2, L, FC, W), BF16),
            dma((3,)), dma((C,)), dma((2, 3)),
        ],
        name="weight_grads",
    )(token_grad, x, g, res)


def shards(tokens, out_grad, route_probs, expert_ids, slot_index, w_gate, w_up, w_down):
    n, e, t = (lax.axis_size(a) for a in ("dp", "expert", "tensor"))
    held, width = tokens.shape
    s = Sizes(n, e, t, held, width, w_gate.shape[0], w_gate.shape[2])
    token_grad, x, g, res = exchange(
        s, tokens, out_grad, route_probs.T, expert_ids.T, slot_index.T, w_gate, w_up, w_down)
    return weight_grads(s, token_grad, x, g, res)


def solution(mesh):
    placed = (
        P(("dp", "expert", "tensor"), None),
        P(("dp", "expert", "tensor"), None),
        P(("dp", "expert"), None),
        P(("dp", "expert"), None),
        P(("dp", "expert"), None),
        P("expert", "dp", "tensor"),
        P("expert", "dp", "tensor"),
        P("expert", "tensor", "dp"),
    )
    return jax.shard_map(
        shards,
        mesh=mesh,
        in_specs=placed,
        out_specs=(
            P(("dp", "expert", "tensor"), None),
            P("expert", "dp", "tensor"),
            P("expert", "dp", "tensor"),
            P("expert", "tensor", "dp"),
        ),
        check_vma=False,
    )
```
